32 devices in a mesh: grp: 2 (over x), seq: 4 (over y, core), tp: 4 (over z).
Axes of the slice: x: 2, y: 2, z: 4, core: 2. Of those that a mesh axis runs over, the one named last changes fastest.
Arguments:
- hidden: bfloat16 [2, 1024, 4096], P('grp', 'seq'), may hold values from -72 to 72
- w_query: bfloat16 [4096, 2048], P('seq', 'tp'), may hold values from -0.09375 to 0.09375
- w_key: bfloat16 [4096, 2048], P('seq', 'tp'), may hold values from -0.09375 to 0.09375
- w_value: bfloat16 [4096, 2048], P('seq', 'tp'), may hold values from -0.09375 to 0.09375
- prompt_len: int32 [256], replicated, may hold values from 1 to 1024
- page_table: int32 [256, 32], replicated, may hold values from 0 to 63, all different within a row
Outputs:
- attended: bfloat16 [2, 1024, 2048], P('grp', 'seq', 'tp')
The draws below stay inside these ranges and needn't reach their ends.
Inputs may be any that keep to these rules, and one draw needn't show every extreme that they name: `page_table`: every row lists 32 different pages; every page is listed by some row.
All inputs are finite; a program needn't handle non-finite values.
Results may differ from the reference program's by a relative error of at most 0.006.
The reference program's roundings to bfloat16 on the way count: a program that leaves them out, or rounds other values in their place, can miss the bound.
Values may be sent and summed in bfloat16 or wider, within the bound.
A program may use at most 128 MiB of HBM per device.

```python
import math
import jax
import jax.numpy as jnp
from jax import lax

D = 4096
HEADS = 16
HD = 128
PAGE = 16
STEPS = 4
ROWS = 256
PROMPT = 1024
PAGES = 64
CTXP = 32


def draw_hidden(key, part):
    base = jnp.clip(jax.random.normal(key, (2, PROMPT, D), jnp.float32), -6.0, 6.0)
    return base.astype(jnp.bfloat16)


def place_ends(values, stream_key, smallest, largest):
    longest = values.shape.index(max(values.shape))
    spots = []
    for shift in (0, 1):
        where = [jax.random.randint(jax.random.fold_in(stream_key, axis), (), 0, length) for axis, length in enumerate(values.shape)]
        where[longest] = (where[longest] + shift) % values.shape[longest]
        spots.append(tuple(where))
    return values.at[spots[0]].set(smallest).at[spots[1]].set(largest)


def block_levels(key, shape, cuts, least, high):
    factor_of = 1.0
    for dim, blocks in cuts:
        draws = jax.random.uniform(jax.random.fold_in(jax.random.fold_in(key, 6), dim), (blocks,), jnp.float32, least / len(cuts), high / len(cuts))
        factor_of = factor_of * jnp.repeat(jnp.exp(draws), shape[dim] // blocks).reshape((-1,) + (1,) * (len(shape) - 1 - dim))
    return factor_of


def different_ones(key, rows, amount, top, lift):
    ranking = jax.random.permutation(jax.random.fold_in(key, 1), amount)
    boost = ranking
    for power in range(3):
        boost = boost * boost // amount
    boost = boost * lift // amount
    chance = jax.random.randint(jax.random.fold_in(key, 2), (rows, amount), 0, 4096) + boost
    sure = jax.random.permutation(jax.random.fold_in(key, 3), rows)[jnp.arange(amount) % rows]
    chance = jnp.where(jnp.arange(rows)[:, None] == sure[None, :], 1 << 14, chance)
    score = chance * amount + jnp.arange(amount)
    return lax.top_k(score.astype(jnp.int32), top)[1].astype(jnp.int32)


def gaussian(stream_key, shape, deviation, reach, cuts=(), kind=jnp.bfloat16):
    loudness = block_levels(stream_key, shape, cuts, -0.22, 0.18) if cuts else 1.0
    values = jax.random.normal(stream_key, shape, jnp.float32) * deviation * loudness
    return jnp.minimum(jnp.maximum(values, -reach), reach).astype(kind)


def setup_inputs(seed: int = 0) -> dict:
    key_of = jax.random.split(jax.random.key(seed), 7)
    hidden = draw_hidden(jax.random.fold_in(key_of[6], 71), 0)
    w_query = gaussian(key_of[1], (D, HEADS * HD), D ** -0.5, 0.09375, ((0, 4), (1, 4)))
    w_key = gaussian(key_of[2], (D, HEADS * HD), D ** -0.5, 0.09375, ((0, 4), (1, 4)))
    w_value = gaussian(key_of[3], (D, HEADS * HD), D ** -0.5, 0.09375, ((0, 4), (1, 4)))
    prompt_len = place_ends(jax.random.randint(key_of[4], (ROWS,), 1, PROMPT + 1), jax.random.fold_in(key_of[4], 1), 1, PROMPT).astype(jnp.int32)
    page_table = different_ones(key_of[5], ROWS, PAGES, CTXP, 4096)
    return {"hidden": hidden, "w_query": w_query, "w_key": w_key, "w_value": w_value, "prompt_len": prompt_len, "page_table": page_table}


NEG = -1.0e30


def attend_head(query, keys, values, allowed):
    scores = jnp.dot(query, keys.T, preferred_element_type=jnp.float32) * (HD ** -0.5)
    scores = jnp.where(allowed, scores, NEG)
    top = jnp.max(scores, axis=1, keepdims=True)
    weights = jnp.where(allowed, jnp.exp(scores - top), 0.0)
    total = jnp.sum(weights, axis=1, keepdims=True)
    summed = jnp.dot(weights.astype(jnp.bfloat16), values, preferred_element_type=jnp.float32)
    return summed / total


def reference(hidden, w_query, w_key, w_value, prompt_len, page_table):
    flat_hidden = hidden.reshape(2 * PROMPT, D)

    def project(weight):
        out = jnp.dot(flat_hidden, weight, preferred_element_type=jnp.float32).astype(jnp.bfloat16)
        return out.reshape(2, PROMPT, HEADS, HD)

    query, keys, values = project(w_query), project(w_key), project(w_value)
    qblock = math.gcd(PROMPT, 512)

    def prefill_head(head):
        head_query, head_keys, head_values = head
        pieces = []
        for index in range(PROMPT // qblock):
            begin = index * qblock
            end = begin + qblock
            query_pos = jnp.arange(begin, end).astype(jnp.int32)
            key_pos = jnp.arange(end).astype(jnp.int32)
            allowed = key_pos[None, :] <= query_pos[:, None]
            pieces.append(attend_head(head_query[begin:end], head_keys[:end], head_values[:end], allowed))
        return jnp.concatenate(pieces, axis=0).astype(jnp.bfloat16)

    prefill = lax.map(prefill_head, (query[0].transpose(1, 0, 2), keys[0].transpose(1, 0, 2), values[0].transpose(1, 0, 2)))
    prefill = prefill.transpose(1, 0, 2).reshape(PROMPT, HEADS * HD)

    rblock = math.gcd(ROWS, 8)
    offsets = jnp.arange(PAGE).astype(jnp.int32)
    causal_steps = jnp.arange(STEPS)[None, :] <= jnp.arange(STEPS)[:, None]

    def decode_block(index):
        first_row = index * rblock
        tables = lax.dynamic_slice_in_dim(page_table, first_row, rblock, 0)
        lengths = lax.dynamic_slice_in_dim(prompt_len, first_row, rblock, 0)
        key_pos = (tables[:, :, None] * PAGE + offsets[None, None, :]).reshape(rblock, CTXP * PAGE)
        context_allowed = key_pos < lengths[:, None]
        context_keys = keys[0][key_pos]
        context_values = values[0][key_pos]
        first_pos = first_row * STEPS
        block_query = lax.dynamic_slice_in_dim(query[1], first_pos, rblock * STEPS, 0).reshape(rblock, STEPS, HEADS, HD)
        own_keys = lax.dynamic_slice_in_dim(keys[1], first_pos, rblock * STEPS, 0).reshape(rblock, STEPS, HEADS, HD)
        own_values = lax.dynamic_slice_in_dim(values[1], first_pos, rblock * STEPS, 0).reshape(rblock, STEPS, HEADS, HD)
        all_keys = jnp.concatenate([context_keys, own_keys], axis=1)
        all_values = jnp.concatenate([context_values, own_values], axis=1)
        allowed = jnp.concatenate([
            jnp.broadcast_to(context_allowed[:, None, :], (rblock, STEPS, CTXP * PAGE)),
            jnp.broadcast_to(causal_steps[None], (rblock, STEPS, STEPS))], axis=2)
        scores = jnp.einsum("rshd,rkhd->rhsk", block_query.astype(jnp.float32), all_keys.astype(jnp.float32)) * (HD ** -0.5)
        scores = jnp.where(allowed[:, None], scores, NEG)
        top = jnp.max(scores, axis=3, keepdims=True)
        weights = jnp.where(allowed[:, None], jnp.exp(scores - top), 0.0)
        total = jnp.sum(weights, axis=3)
        summed = jnp.einsum("rhsk,rkhd->rshd", weights.astype(jnp.bfloat16).astype(jnp.float32), all_values.astype(jnp.float32))
        result = summed / total.transpose(0, 2, 1)[:, :, :, None]
        return result.reshape(rblock * STEPS, HEADS * HD).astype(jnp.bfloat16)

    decode = lax.map(decode_block, jnp.arange(ROWS // rblock).astype(jnp.int32)).reshape(PROMPT, HEADS * HD)
    return jnp.stack([prefill, decode])
```

```python
import math

import jax
import jax.numpy as jnp
from jax import lax
from jax.experimental import pallas as pl
from jax.experimental.pallas import tpu as pltpu
from jax.sharding import PartitionSpec as P

HD = 128
PAGE = 16
STEPS = 4


NEG = -1e30


def from_behind(value, axis, steps):
    count = lax.axis_size(axis)
    first, last = (max(0, -steps), min(count, count - steps))
    return lax.ppermute(value, axis, [(source, source + steps) for source in range(first, last)])


def partial_attention(query, keys, values, allowed):
    rows = query.shape[0]
    heads = query.shape[1] // HD
    query_heads = query.reshape(rows, heads, HD)
    key_heads = keys.reshape(keys.shape[0], heads, HD)
    value_heads = values.reshape(values.shape[0], heads, HD)
    scores = jnp.einsum(
        "rhd,shd->hrs", query_heads, key_heads, preferred_element_type=jnp.float32
    ) * HD ** (-0.5)
    scores = jnp.where(allowed[None], scores, NEG)
    top = jnp.max(scores, axis=2)
    weights = jnp.where(allowed[None], jnp.exp(scores - top[:, :, None]), 0.0)
    total = jnp.sum(weights, axis=2)
    summed = jnp.einsum(
        "hrs,shd->rhd",
        weights.astype(jnp.bfloat16),
        value_heads,
        preferred_element_type=jnp.float32,
    )
    return (top, total, summed.reshape(rows, heads * HD))


def rescale(summed, factor):
    rows = summed.shape[0]
    heads = factor.shape[0]
    return (summed.reshape(rows, heads, HD) * factor.T[:, :, None]).reshape(rows, heads * HD)


def combine(first, second):
    top = jnp.maximum(first[0], second[0])
    early = jnp.exp(first[0] - top)
    later = jnp.exp(second[0] - top)
    return (
        top,
        first[1] * early + second[1] * later,
        rescale(first[2], early) + rescale(second[2], later),
    )


def finish(state):
    return rescale(state[2], 1.0 / state[1]).astype(jnp.bfloat16)


def row_mask(tables, lengths, key_pos):
    pages = key_pos // PAGE
    member = jnp.any(tables[:, :, None] == pages[None, None, :], axis=1)
    allowed = member & (key_pos[None, :] < lengths[:, None])
    return jnp.repeat(allowed, STEPS, axis=0)


def blocked(carry, keys, values, query, mask_of):
    count = keys.shape[0]
    block = math.gcd(count, 512)

    def one_block(state, offset):
        piece_keys = lax.dynamic_slice_in_dim(keys, offset, block, 0)
        piece_values = lax.dynamic_slice_in_dim(values, offset, block, 0)
        key_pos = offset + jnp.arange(block)
        return (
            combine(state, partial_attention(query, piece_keys, piece_values, mask_of(key_pos))),
            None,
        )

    offsets = jnp.arange(count // block) * block
    state, unused = lax.scan(one_block, carry, offsets)
    return state


def on_device(hidden, w_query, w_key, w_value, prompt_len, page_table):
    local = hidden[0]
    rows = local.shape[0]
    width = w_query.shape[1]
    heads = width // HD
    seq_index = lax.axis_index("seq")
    is_prompt = lax.axis_index("grp") == 0
    empty = jnp.zeros((rows, width), jnp.float32)
    piece = (
        lax.all_gather(w_query, "seq", axis=0, tiled=True),
        lax.all_gather(w_key, "seq", axis=0, tiled=True),
        lax.all_gather(w_value, "seq", axis=0, tiled=True),
    )
    projected = tuple(
        (jnp.dot(local, weight, preferred_element_type=jnp.float32) for weight in piece)
    )
    query, keys, values = [item.astype(jnp.bfloat16) for item in projected]
    positions = seq_index * rows + jnp.arange(rows)
    start_state = (
        jnp.full((heads, rows), NEG, jnp.float32),
        jnp.zeros((heads, rows), jnp.float32),
        empty,
    )
    given_keys, given_values = from_behind((keys, values), "grp", 1)
    cache_keys = jnp.where(is_prompt, keys, given_keys)
    cache_values = jnp.where(is_prompt, values, given_values)
    row_count = rows // STEPS
    own_tables = lax.dynamic_slice_in_dim(page_table, seq_index * row_count, row_count, 0)
    own_lengths = lax.dynamic_slice_in_dim(prompt_len, seq_index * row_count, row_count, 0)

    def mask_of(key_pos):
        causal = key_pos[None, :] <= positions[:, None]
        listed = row_mask(own_tables, own_lengths, key_pos)
        return jnp.where(is_prompt, causal, listed)

    piece = (
        lax.all_gather(cache_keys, "seq", axis=0, tiled=True),
        lax.all_gather(cache_values, "seq", axis=0, tiled=True),
    )
    state = blocked(start_state, piece[0], piece[1], query, mask_of)
    frame_row = positions // STEPS
    own_rows = (frame_row[:, None] == frame_row[None, :]) & (
        positions[None, :] <= positions[:, None]
    )
    fresh = partial_attention(query, keys, values, own_rows)
    prefill_out = finish(state)
    decode_out = finish(combine(state, fresh))
    return jnp.where(is_prompt, prefill_out, decode_out)[None]


QUERY, KEY, VALUE = 0, 1, 2
PROMPT, DECODE = 0, 1
CHUNKS = 8
KV_PIECES = 2


def fused_kernel(
    hidden, w_query, w_key, w_value, lengths_in, tables_in, out,
    lengths, tables, states, kv_weights, q_weights, kv_acc, q_acc, own_kv, far_kv, qbuf,
    near_bias, far_bias, near_scores, fresh_scores, far_part, near_part, totals, osend, orecv,
    local_sem, d_send, d_recv, y_send, y_recv, hd_send, hd_recv, hx_send, hx_recv, hz_send, hz_recv,
    hp_send, hp_recv, k_send, k_recv, o_send, o_recv,
):
    inputs = {QUERY: w_query, KEY: w_key, VALUE: w_value}
    order = (KEY, VALUE, QUERY)
    rows = hidden.shape[1]
    depth = w_query.shape[0]
    half_rows = rows // 2
    chunk = half_rows // CHUNKS
    chip_rows = 2 * rows
    block = rows // 2
    blocks = chip_rows // block
    grp = lax.axis_index("grp")
    seq = lax.axis_index("seq")
    tp = lax.axis_index("tp")
    y = seq // 2
    core = seq % 2
    side = tp % 2
    partner = {"seq": 2 * y + 1 - core}
    across = [{"seq": 2 * (1 - y) + core}, {"seq": 2 * (1 - y) + 1 - core}]
    beside = [{"grp": 1 - grp, "seq": 2 * y + core}, {"grp": 1 - grp, "seq": 2 * y + 1 - core}]
    above = {"tp": tp + 1 - 2 * side}
    cores = [core, 1 - core]

    def remote(src, dst, send, recv, to):
        return pltpu.make_async_remote_copy(
            src_ref=src, dst_ref=dst, send_sem=send, recv_sem=recv,
            device_id=to, device_id_type=pl.DeviceIdType.MESH,
        )

    def head_lanes(of_grp, of_core):
        return pl.ds(pl.multiple_of((2 * of_grp + of_core) * HD, HD), HD)

    def quarter(of_seq):
        return pl.ds(pl.multiple_of(of_seq * depth, depth), depth)

    def landing(m, of_seq):
        if m == QUERY:
            return q_weights.at[quarter(of_seq)]
        return kv_weights.at[quarter(of_seq), (m - KEY) * HD : (m - KEY + 1) * HD]

    keeps = {
        m: pltpu.make_async_copy(inputs[m].at[:, head_lanes(grp, core)], landing(m, seq), local_sem.at[m])
        for m in order
    }
    table_keep = pltpu.make_async_copy(tables_in, tables, local_sem.at[3])
    length_keep = pltpu.make_async_copy(lengths_in, lengths, local_sem.at[4])
    my_rows = pl.ds(pl.multiple_of(core * rows, rows), rows)
    own_keep = pltpu.make_async_copy(hidden.at[0], states.at[grp, my_rows], local_sem.at[5])
    table_keep.start()
    length_keep.start()
    own_keep.start()
    for m in order:
        keeps[m].start()

    barrier = pltpu.get_barrier_semaphore()
    for peer in (partner, *across, *beside, above):
        pl.semaphore_signal(barrier, inc=1, device_id=peer, device_id_type=pl.DeviceIdType.MESH)
    pl.semaphore_wait(barrier, 6)

    sent = []

    def launch(copy):
        copy.start()
        sent.append(copy)

    def y_weight(m, rel):
        at = m * 2 + rel
        return remote(
            inputs[m].at[:, head_lanes(grp, cores[rel])], landing(m, seq), y_send.at[at], y_recv.at[at], across[rel]
        )

    def y_arrival(m, rel):
        at = m * 2 + rel
        spot = landing(m, 2 * (1 - y) + cores[rel])
        return remote(spot, spot, y_send.at[at], y_recv.at[at], across[rel])

    def chunk_rows(which, of_core, at):
        return pl.ds(pl.multiple_of(of_core * rows + which * half_rows + at * chunk, chunk), chunk)

    def x_chunk(at):
        source = pl.ds(pl.multiple_of(side * half_rows + at * chunk, chunk), chunk)
        return remote(
            hidden.at[0, source], states.at[grp, chunk_rows(side, core, at)],
            hx_send.at[at], hx_recv.at[at], beside[0],
        )

    def x_arrival(at):
        spot = states.at[1 - grp, chunk_rows(side, core, at)]
        return remote(spot, spot, hx_send.at[at], hx_recv.at[at], beside[0])

    def z_chunk(at):
        spot = states.at[1 - grp, chunk_rows(side, core, at)]
        return remote(spot, spot, hz_send.at[at], hz_recv.at[at], above)

    def z_arrival(at):
        spot = states.at[1 - grp, chunk_rows(1 - side, core, at)]
        return remote(spot, spot, hz_send.at[at], hz_recv.at[at], above)

    def relay_chunk(which, at, of_core):
        spot = states.at[1 - grp, chunk_rows(side if which == 0 else 1 - side, of_core, at)]
        number = which * CHUNKS + at
        return remote(spot, spot, hp_send.at[number], hp_recv.at[number], partner)

    for m in order:
        for rel in range(2):
            launch(y_weight(m, rel))
    for at in range(CHUNKS):
        launch(x_chunk(at))
    d_weights = {
        m: remote(inputs[m].at[:, head_lanes(grp, 1 - core)], landing(m, seq), d_send.at[m], d_recv.at[m], partner)
        for m in order
    }
    own_swap = remote(hidden.at[0], states.at[grp, my_rows], hd_send, hd_recv, partner)
    launch(d_weights[KEY])
    launch(d_weights[VALUE])
    launch(own_swap)
    launch(d_weights[QUERY])

    table_keep.wait()
    length_keep.wait()
    decode_rows = chip_rows // STEPS
    pages = 2 * chip_rows // PAGE
    own_rows = pl.ds(pl.multiple_of(y * decode_rows, decode_rows), decode_rows)
    own_table = tables[:, own_rows]
    own_length = lengths[:, own_rows]
    page_row = lax.broadcasted_iota(jnp.int32, (pages, decode_rows), 0)
    member = own_table[0:1, :] == page_row
    for listed in range(1, own_table.shape[0]):
        member = member | (own_table[listed : listed + 1, :] == page_row)
    member = jnp.where(member, 1.0, 0.0).astype(jnp.bfloat16)
    step_bits = STEPS.bit_length() - 1
    page_bits = PAGE.bit_length() - 1
    spread = (
        lax.shift_right_logical(lax.broadcasted_iota(jnp.int32, (chip_rows, decode_rows), 0), step_bits)
        == lax.broadcasted_iota(jnp.int32, (chip_rows, decode_rows), 1)
    )
    spread = jnp.where(spread, 1.0, 0.0).astype(jnp.bfloat16)
    contract_last = (((1,), (1,)), ((), ()))
    for which, bias in enumerate((near_bias, far_bias)):
        base = (y if which == 0 else 1 - y) * chip_rows
        key_page = lax.shift_right_logical(
            lax.broadcasted_iota(jnp.int32, (chip_rows, pages), 0) + base, page_bits
        )
        unfold = lax.broadcasted_iota(jnp.int32, (chip_rows, pages), 1) == key_page
        unfold = jnp.where(unfold, 1.0, 0.0).astype(jnp.bfloat16)
        seen = jnp.dot(unfold, member, preferred_element_type=jnp.float32)
        key_pos = lax.broadcasted_iota(jnp.int32, (chip_rows, decode_rows), 0) + base
        seen = jnp.where(key_pos < own_length, seen, 0.0).astype(jnp.bfloat16)
        listed = lax.dot_general(spread, seen, contract_last, preferred_element_type=jnp.float32)
        bias[...] = jnp.where(listed > 0.5, 0.0, NEG)

    def kv_dot(group, of_seq):
        return jnp.dot(
            states[group, :, quarter(of_seq)], kv_weights[quarter(of_seq), :], preferred_element_type=jnp.float32
        )

    def q_dot(group, of_seq):
        return jnp.dot(
            states[group, :, quarter(of_seq)], q_weights[quarter(of_seq), :], preferred_element_type=jnp.float32
        )

    near_seqs = [seq, 2 * y + 1 - core]
    far_seqs = [2 * (1 - y) + core, 2 * (1 - y) + 1 - core]

    def take_x(at):
        x_arrival(at).wait_recv()
        launch(z_chunk(at))
        launch(relay_chunk(0, at, core))

    def take_z(at):
        z_arrival(at).wait_recv()
        launch(relay_chunk(1, at, core))

    def near_kv():
        own_keep.wait()
        own_swap.wait_recv()
        for m in (KEY, VALUE):
            keeps[m].wait()
            d_weights[m].wait_recv()
        kv_acc[grp] = kv_dot(grp, near_seqs[0]) + kv_dot(grp, near_seqs[1])

    def near_q():
        keeps[QUERY].wait()
        d_weights[QUERY].wait_recv()
        q_acc[grp] = q_dot(grp, near_seqs[0]) + q_dot(grp, near_seqs[1])

    def far_kv_dot(rel):
        for m in (KEY, VALUE):
            y_arrival(m, rel).wait_recv()
        kv_acc[grp] += kv_dot(grp, far_seqs[rel])

    LATE = 2
    for at in range(CHUNKS + LATE):
        if at < CHUNKS:
            take_x(at)
        if at >= LATE:
            take_z(at - LATE)
        if at == 0:
            near_kv()
        if at == 1:
            near_q()
    for rel in range(2):
        far_kv_dot(rel)
    for which in range(2):
        for at in range(CHUNKS):
            relay_chunk(which, at, 1 - core).wait_recv()
    other = 1 - grp
    kv_acc[other] = (kv_dot(other, near_seqs[0]) + kv_dot(other, near_seqs[1])) + (
        kv_dot(other, far_seqs[0]) + kv_dot(other, far_seqs[1])
    )
    for group in (PROMPT, DECODE):
        for kind in range(2):
            own_kv[group, kind] = kv_acc[group, :, kind * HD : (kind + 1) * HD].astype(jnp.bfloat16)

    def kv_copy(kind, piece):
        span = pl.ds(piece * (chip_rows // KV_PIECES), chip_rows // KV_PIECES)
        at = kind * KV_PIECES + piece
        return remote(
            own_kv.at[PROMPT, kind, span], far_kv.at[kind, span], k_send.at[at], k_recv.at[at], across[0]
        )

    for kind in range(2):
        for piece in range(KV_PIECES):
            launch(kv_copy(kind, piece))
    q_acc[other] = q_dot(other, near_seqs[0]) + q_dot(other, near_seqs[1])
    for rel in range(2):
        y_arrival(QUERY, rel).wait_recv()
        if rel == 0:
            for group in (PROMPT, DECODE):
                q_acc[group] += q_dot(group, far_seqs[rel])
        else:
            for group in (PROMPT, DECODE):
                qbuf[group] = (q_acc[group] + q_dot(group, far_seqs[rel])).astype(jnp.bfloat16)

    scale = HD ** (-0.5)
    fresh_row = lax.broadcasted_iota(jnp.int32, (block, block), 0)
    fresh_col = lax.broadcasted_iota(jnp.int32, (block, block), 1)
    same = (
        lax.shift_right_logical(fresh_row, step_bits) == lax.shift_right_logical(fresh_col, step_bits)
    ) & (fresh_col <= fresh_row)
    fresh_bias = jnp.where(same, 0.0, NEG)
    far_prompt_bias = jnp.where(y == 1, 0.0, NEG)

    def product(group, span, keys):
        return lax.dot_general(
            qbuf[group, span], keys, contract_last, preferred_element_type=jnp.float32
        ) * scale

    for at in range(blocks):
        span = slice(at * block, (at + 1) * block)
        causal = (
            lax.broadcasted_iota(jnp.int32, (block, chip_rows), 1)
            <= lax.broadcasted_iota(jnp.int32, (block, chip_rows), 0) + at * block
        )
        near_scores[PROMPT, span] = jnp.where(causal, product(PROMPT, span, own_kv[PROMPT, 0]), NEG)
        near_scores[DECODE, span] = product(DECODE, span, own_kv[PROMPT, 0]) + near_bias[span]
        fresh_scores[span] = product(DECODE, span, own_kv[DECODE, 0, span]) + fresh_bias

    for piece in range(KV_PIECES):
        kv_copy(0, piece).wait_recv()

    def weigh(group, at):
        span = slice(at * block, (at + 1) * block)
        far_score = product(group, span, far_kv[0])
        far_score = far_score + (far_prompt_bias if group == PROMPT else far_bias[span])
        near_score = near_scores[group, span]
        top = jnp.maximum(jnp.max(near_score, axis=1, keepdims=True), jnp.max(far_score, axis=1, keepdims=True))
        if group == DECODE:
            top = jnp.maximum(top, jnp.max(fresh_scores[span], axis=1, keepdims=True))
        near = jnp.exp(near_score - top)
        far = jnp.exp(far_score - top)
        total = jnp.sum(near, axis=1, keepdims=True) + jnp.sum(far, axis=1, keepdims=True)
        summed = jnp.dot(near.astype(jnp.bfloat16), own_kv[PROMPT, 1], preferred_element_type=jnp.float32)
        if group == DECODE:
            fresh = jnp.exp(fresh_scores[span] - top)
            total += jnp.sum(fresh, axis=1, keepdims=True)
            summed += jnp.dot(
                fresh.astype(jnp.bfloat16), own_kv[DECODE, 1, span], preferred_element_type=jnp.float32
            )
        far_part[group, span] = far.astype(jnp.bfloat16)
        near_part[group, span] = summed
        totals[group, span] = jnp.broadcast_to(total, (block, HD))

    for at in range(blocks):
        for group in (PROMPT, DECODE):
            weigh(group, at)
    for piece in range(KV_PIECES):
        kv_copy(1, piece).wait_recv()

    def attended(group, of_core, at):
        span = pl.ds(pl.multiple_of(of_core * rows + at * block, block), block)
        summed = near_part[group, span] + jnp.dot(
            far_part[group, span], far_kv[1], preferred_element_type=jnp.float32
        )
        return (summed / totals[group, span]).astype(jnp.bfloat16)

    pieces = rows // block

    def out_copy(source, at):
        number = source * pieces + at
        span = pl.ds(at * block, block)
        to = (partner, beside[0], beside[1])[source]
        return remote(
            osend.at[source, span], orecv.at[source, span], o_send.at[number], o_recv.at[number], to
        )

    for source in (2, 1):
        for at in range(pieces):
            osend[source, at * block : (at + 1) * block] = attended(other, cores[source - 1], at)
            launch(out_copy(source, at))
    for at in range(pieces):
        osend[0, at * block : (at + 1) * block] = attended(grp, 1 - core, at)
        launch(out_copy(0, at))
    for at in range(pieces):
        out[at * block : (at + 1) * block, head_lanes(grp, core)] = attended(grp, core, at)
    for source in (0, 2, 1):
        lanes = (head_lanes(grp, 1 - core), head_lanes(other, core), head_lanes(other, 1 - core))[source]
        for at in range(pieces):
            out_copy(source, at).wait_recv()
            out[at * block : (at + 1) * block, lanes] = orecv[source, at * block : (at + 1) * block]

    for copy in sent:
        copy.wait_send()


def fused(hidden, w_query, w_key, w_value, prompt_len, page_table):
    rows, model = hidden.shape[1:]
    depth, width = w_query.shape
    chip_rows = 2 * rows
    block = rows // 2
    dma = pltpu.SemaphoreType.DMA
    anywhere = pl.BlockSpec(memory_space=pltpu.HBM)
    vmem = pl.BlockSpec(memory_space=pltpu.VMEM)
    pieces = rows // block
    result = pl.pallas_call(
        fused_kernel,
        out_shape=jax.ShapeDtypeStruct((rows, width), jnp.bfloat16),
        in_specs=[anywhere] * 6,
        out_specs=vmem,
        scratch_shapes=[
            pltpu.VMEM((1, prompt_len.shape[0]), jnp.int32),
            pltpu.VMEM(page_table.shape[::-1], jnp.int32),
            pltpu.VMEM((2, chip_rows, model), jnp.bfloat16),
            pltpu.VMEM((model, 2 * HD), jnp.bfloat16),
            pltpu.VMEM((model, HD), jnp.bfloat16),
            pltpu.VMEM((2, chip_rows, 2 * HD), jnp.float32),
            pltpu.VMEM((2, chip_rows, HD), jnp.float32),
            pltpu.VMEM((2, 2, chip_rows, HD), jnp.bfloat16),
            pltpu.VMEM((2, chip_rows, HD), jnp.bfloat16),
            pltpu.VMEM((2, chip_rows, HD), jnp.bfloat16),
            pltpu.VMEM((chip_rows, chip_rows), jnp.float32),
            pltpu.VMEM((chip_rows, chip_rows), jnp.float32),
            pltpu.VMEM((2, chip_rows, chip_rows), jnp.float32),
            pltpu.VMEM((chip_rows, block), jnp.float32),
            pltpu.VMEM((2, chip_rows, chip_rows), jnp.bfloat16),
            pltpu.VMEM((2, chip_rows, HD), jnp.float32),
            pltpu.VMEM((2, chip_rows, HD), jnp.float32),
            pltpu.VMEM((3, rows, HD), jnp.bfloat16),
            pltpu.VMEM((3, rows, HD), jnp.bfloat16),
            dma((6,)), dma((3,)), dma((3,)), dma((6,)), dma((6,)), dma(()), dma(()),
            dma((CHUNKS,)), dma((CHUNKS,)), dma((CHUNKS,)), dma((CHUNKS,)),
            dma((2 * CHUNKS,)), dma((2 * CHUNKS,)),
            dma((2 * KV_PIECES,)), dma((2 * KV_PIECES,)),
            dma((3 * pieces,)), dma((3 * pieces,)),
        ],
        compiler_params=pltpu.CompilerParams(
            collective_id=0, has_side_effects=True, vmem_limit_bytes=67043328
        ),
    )(hidden, w_query, w_key, w_value, prompt_len.reshape(1, -1), page_table.T)
    return result[None]


def solution(mesh):
    paired = mesh.shape["grp"] == 2 and mesh.shape["seq"] == 4 and mesh.shape["tp"] % 2 == 0
    return jax.shard_map(
        fused if paired else on_device,
        mesh=mesh,
        in_specs=(P("grp", "seq", None), P("seq", "tp"), P("seq", "tp"), P("seq", "tp"), P(), P()),
        out_specs=P("grp", "seq", "tp"),
        check_vma=False,
    )
```

```python
import functools
import math

import jax
import jax.numpy as jnp
from jax import lax
from jax.experimental import pallas as pl
from jax.experimental.pallas import tpu as pltpu
from jax.sharding import PartitionSpec as P

HD = 128
PAGE = 16
STEPS = 4


NEG = -1e30


def from_behind(value, axis, steps):
    count = lax.axis_size(axis)
    first, last = (max(0, -steps), min(count, count - steps))
    return lax.ppermute(value, axis, [(source, source + steps) for source in range(first, last)])


def partial_attention(query, keys, values, allowed):
    rows = query.shape[0]
    heads = query.shape[1] // HD
    query_heads = query.reshape(rows, heads, HD)
    key_heads = keys.reshape(keys.shape[0], heads, HD)
    value_heads = values.reshape(values.shape[0], heads, HD)
    scores = jnp.einsum(
        "rhd,shd->hrs", query_heads, key_heads, preferred_element_type=jnp.float32
    ) * HD ** (-0.5)
    scores = jnp.where(allowed[None], scores, NEG)
    top = jnp.max(scores, axis=2)
    weights = jnp.where(allowed[None], jnp.exp(scores - top[:, :, None]), 0.0)
    total = jnp.sum(weights, axis=2)
    summed = jnp.einsum(
        "hrs,shd->rhd",
        weights.astype(jnp.bfloat16),
        value_heads,
        preferred_element_type=jnp.float32,
    )
    return (top, total, summed.reshape(rows, heads * HD))


def rescale(summed, factor):
    rows = summed.shape[0]
    heads = factor.shape[0]
    return (summed.reshape(rows, heads, HD) * factor.T[:, :, None]).reshape(rows, heads * HD)


def combine(first, second):
    top = jnp.maximum(first[0], second[0])
    early = jnp.exp(first[0] - top)
    later = jnp.exp(second[0] - top)
    return (
        top,
        first[1] * early + second[1] * later,
        rescale(first[2], early) + rescale(second[2], later),
    )


def finish(state):
    return rescale(state[2], 1.0 / state[1]).astype(jnp.bfloat16)


def row_mask(tables, lengths, key_pos):
    pages = key_pos // PAGE
    member = jnp.any(tables[:, :, None] == pages[None, None, :], axis=1)
    allowed = member & (key_pos[None, :] < lengths[:, None])
    return jnp.repeat(allowed, STEPS, axis=0)


def blocked(carry, keys, values, query, mask_of):
    count = keys.shape[0]
    block = math.gcd(count, 512)

    def one_block(state, offset):
        piece_keys = lax.dynamic_slice_in_dim(keys, offset, block, 0)
        piece_values = lax.dynamic_slice_in_dim(values, offset, block, 0)
        key_pos = offset + jnp.arange(block)
        return (
            combine(state, partial_attention(query, piece_keys, piece_values, mask_of(key_pos))),
            None,
        )

    offsets = jnp.arange(count // block) * block
    state, unused = lax.scan(one_block, carry, offsets)
    return state


def on_device(hidden, w_query, w_key, w_value, prompt_len, page_table):
    local = hidden[0]
    rows = local.shape[0]
    width = w_query.shape[1]
    heads = width // HD
    seq_index = lax.axis_index("seq")
    is_prompt = lax.axis_index("grp") == 0
    empty = jnp.zeros((rows, width), jnp.float32)
    piece = (
        lax.all_gather(w_query, "seq", axis=0, tiled=True),
        lax.all_gather(w_key, "seq", axis=0, tiled=True),
        lax.all_gather(w_value, "seq", axis=0, tiled=True),
    )
    projected = tuple(
        (jnp.dot(local, weight, preferred_element_type=jnp.float32) for weight in piece)
    )
    query, keys, values = [item.astype(jnp.bfloat16) for item in projected]
    positions = seq_index * rows + jnp.arange(rows)
    start_state = (
        jnp.full((heads, rows), NEG, jnp.float32),
        jnp.zeros((heads, rows), jnp.float32),
        empty,
    )
    given_keys, given_values = from_behind((keys, values), "grp", 1)
    cache_keys = jnp.where(is_prompt, keys, given_keys)
    cache_values = jnp.where(is_prompt, values, given_values)
    row_count = rows // STEPS
    own_tables = lax.dynamic_slice_in_dim(page_table, seq_index * row_count, row_count, 0)
    own_lengths = lax.dynamic_slice_in_dim(prompt_len, seq_index * row_count, row_count, 0)

    def mask_of(key_pos):
        causal = key_pos[None, :] <= positions[:, None]
        listed = row_mask(own_tables, own_lengths, key_pos)
        return jnp.where(is_prompt, causal, listed)

    piece = (
        lax.all_gather(cache_keys, "seq", axis=0, tiled=True),
        lax.all_gather(cache_values, "seq", axis=0, tiled=True),
    )
    state = blocked(start_state, piece[0], piece[1], query, mask_of)
    frame_row = positions // STEPS
    own_rows = (frame_row[:, None] == frame_row[None, :]) & (
        positions[None, :] <= positions[:, None]
    )
    fresh = partial_attention(query, keys, values, own_rows)
    prefill_out = finish(state)
    decode_out = finish(combine(state, fresh))
    return jnp.where(is_prompt, prefill_out, decode_out)[None]


QUERY, KEY, VALUE = 0, 1, 2
OWN, OTHER = 0, 1
SUBS = 2


def fused_kernel(
    planes, hidden, w_query, w_key, w_value, lengths_in, tables_in, out,
    lengths, tables, own, other, weights, acc, wide_out, wide_in, value_out, value_in, qbuf, fresh, cache, bias, osend, orecv,
    local_sem, w_send, w_recv, hy_send, hy_recv, up_send, down_send, hz_recv, p_send, p_recv,
    kx_send, kx_recv, kd_send, kd_recv, o_send, o_recv,
):
    inputs = {QUERY: w_query, KEY: w_key, VALUE: w_value}
    rows = hidden.shape[1]
    depth, width = w_query.shape
    span = 2 * depth
    half = width // 2
    heads = half // HD
    block = rows // 2
    chunk = rows // planes // SUBS
    grp = lax.axis_index("grp")
    seq = lax.axis_index("seq")
    tp = lax.axis_index("tp")
    y = seq // 2
    core = seq % 2
    side = tp // (planes // 2)
    partner = {"seq": 2 * y + 1 - core}
    across = {"seq": 2 * (1 - y) + core}
    beside = {"grp": 1 - grp}
    above = {"tp": lax.rem(tp + 1, planes)}
    below = {"tp": lax.rem(tp + planes - 1, planes)}
    kinds = {KEY: 0, VALUE: 1}
    seqs = [2 * y + core, 2 * (1 - y) + core]
    my_heads = pl.ds(pl.multiple_of(y * half, half), half)
    their_heads = pl.ds(pl.multiple_of((1 - y) * half, half), half)
    halves = [pl.ds(pl.multiple_of(at * block, block), block) for at in (side, 1 - side)]

    def remote(src, dst, send, recv, to):
        return pltpu.make_async_remote_copy(
            src_ref=src, dst_ref=dst, send_sem=send, recv_sem=recv,
            device_id=to, device_id_type=pl.DeviceIdType.MESH,
        )

    my_depth = pl.ds(pl.multiple_of(core * depth, depth), depth)
    keeps = {m: pltpu.make_async_copy(inputs[m], weights.at[m, my_depth], local_sem.at[m]) for m in inputs}
    table_keep = pltpu.make_async_copy(tables_in, tables, local_sem.at[3])
    length_keep = pltpu.make_async_copy(lengths_in, lengths, local_sem.at[4])
    own_keep = pltpu.make_async_copy(
        hidden.at[0, :, pl.ds(pl.multiple_of(y * span, span), span)], own, local_sem.at[5]
    )
    table_keep.start()
    length_keep.start()
    own_keep.start()
    for m in (KEY, VALUE, QUERY):
        keeps[m].start()

    barrier = pltpu.get_barrier_semaphore()
    for peer in (across, partner, beside):
        pl.semaphore_signal(barrier, inc=1, device_id=peer, device_id_type=pl.DeviceIdType.MESH)

    @pl.when(tp < planes - 1)
    def _():
        pl.semaphore_signal(barrier, inc=1, device_id=above, device_id_type=pl.DeviceIdType.MESH)

    @pl.when(tp > 0)
    def _():
        pl.semaphore_signal(barrier, inc=1, device_id=below, device_id_type=pl.DeviceIdType.MESH)

    ends = jnp.where(tp == 0, 1, 0) + jnp.where(tp == planes - 1, 1, 0)
    pl.semaphore_wait(barrier, 5 - ends)

    def chunk_rows(plane, sub):
        return pl.ds(pl.multiple_of((plane * SUBS + sub) * chunk, chunk), chunk)

    def y_chunk(sub):
        take = chunk_rows(tp, sub)
        return remote(
            hidden.at[0, take, pl.ds(pl.multiple_of((1 - y) * span, span), span)], other.at[take],
            hy_send.at[sub], hy_recv.at[sub], across,
        )

    def z_chunk(plane, sub, up):
        take = chunk_rows(plane, sub)
        at = plane * SUBS + sub
        return remote(
            other.at[take], other.at[take], (up_send if up else down_send).at[at], hz_recv.at[at],
            above if up else below,
        )

    sent = []

    def launch(copy):
        copy.start()
        sent.append(copy)

    for sub in range(SUBS):
        launch(y_chunk(sub))
    swaps = {
        m: remote(inputs[m], weights.at[m, my_depth], w_send.at[m], w_recv.at[m], partner) for m in inputs
    }
    for m in (KEY, VALUE, QUERY):
        launch(swaps[m])

    table_keep.wait()
    length_keep.wait()
    total_rows = tables.shape[1]
    keys = cache.shape[1]
    pages = keys // PAGE
    decode_rows = rows // STEPS
    step_bits = STEPS.bit_length() - 1
    page_bits = PAGE.bit_length() - 1
    prompt_one = jnp.where(grp == 0, 1, 0)
    contract_last = (((1,), (1,)), ((), ()))
    table = tables[...]
    page_row = lax.broadcasted_iota(jnp.int32, (pages, total_rows), 0)
    member = table[0:1, :] == page_row
    for listed in range(1, table.shape[0]):
        member = member | (table[listed : listed + 1, :] == page_row)
    member = jnp.where(member, 1.0, 0.0).astype(jnp.bfloat16)
    unfold = lax.broadcasted_iota(jnp.int32, (keys, pages), 1) == lax.shift_right_logical(
        lax.broadcasted_iota(jnp.int32, (keys, pages), 0), page_bits
    )
    unfold = jnp.where(unfold, 1.0, 0.0).astype(jnp.bfloat16)
    seen = jnp.dot(unfold, member, preferred_element_type=jnp.float32)
    key_pos = lax.broadcasted_iota(jnp.int32, (keys, total_rows), 0)
    seen = jnp.where(key_pos < lengths[...], seen, 0.0).astype(jnp.bfloat16)
    for s in (OWN, OTHER):
        spread = (
            lax.shift_right_logical(lax.broadcasted_iota(jnp.int32, (rows, total_rows), 0), step_bits)
            + seqs[s] * decode_rows
            == lax.broadcasted_iota(jnp.int32, (rows, total_rows), 1)
        )
        spread = jnp.where(spread, 1.0, 0.0).astype(jnp.bfloat16)
        listed = lax.dot_general(spread, seen, contract_last, preferred_element_type=jnp.float32)
        causal = (
            lax.broadcasted_iota(jnp.int32, (rows, keys), 1)
            <= lax.broadcasted_iota(jnp.int32, (rows, keys), 0) + seqs[s] * rows
        )
        allowed = jnp.where(prompt_one == 1, jnp.where(causal, 1.0, 0.0), listed)
        bias[s] = jnp.where(allowed > 0.5, 0.0, NEG)

    def project(source, at, m, lanes):
        return jnp.dot(source[at, :], weights[m, :, lanes], preferred_element_type=jnp.float32)

    def part_at(wide, narrow, s, m, at):
        return narrow.at[s, at] if m == VALUE else wide.at[s, m, at]

    def send(source, s, at, m):
        spot = part_at(wide_out, value_out, s, m, at)
        spot[...] = project(source, at, m, their_heads).astype(spot.dtype)

    def keep(source, s, at, m):
        acc[s, m, at] = project(source, at, m, my_heads)

    def both(source, s, at, m):
        send(source, s, at, m)
        keep(source, s, at, m)

    def partial(s, m, piece):
        at = halves[piece]
        number = (s * 3 + m) * 2 + piece
        return remote(
            part_at(wide_out, value_out, s, m, at), part_at(wide_in, value_in, 1 - s, m, at),
            p_send.at[number], p_recv.at[number], across,
        )

    everything = pl.ds(0, rows)

    def pass_on(plane, sub, up, down):
        if up:

            @pl.when(tp < planes - 1)
            def _():
                z_chunk(plane, sub, True).start()

        if down:

            @pl.when(tp > 0)
            def _():
                z_chunk(plane, sub, False).start()

    def take_y(sub):
        y_chunk(sub).wait_recv()
        pass_on(tp, sub, True, True)

    def take_z(far):
        for sub in range(SUBS):

            @pl.when(tp + far < planes)
            def _():
                z_chunk(tp + far, sub, False).wait_recv()
                pass_on(tp + far, sub, False, True)

            @pl.when(tp >= far)
            def _():
                z_chunk(tp - far, sub, True).wait_recv()
                pass_on(tp - far, sub, True, False)

    own_keep.wait()
    for at, m in enumerate((KEY, VALUE, QUERY)):
        keeps[m].wait()
        swaps[m].wait_recv()
        if at < SUBS:
            take_y(at)
        for piece in range(2):
            send(own, OWN, halves[piece], m)
            launch(partial(OWN, m, piece))
        keep(own, OWN, everything, m)
    for sub in range(3, SUBS):
        take_y(sub)

    def arrived(s, m, piece):
        at = halves[piece]
        remote(
            part_at(wide_out, value_out, s, m, at), part_at(wide_in, value_in, s, m, at),
            p_send.at[((1 - s) * 3 + m) * 2 + piece], p_recv.at[((1 - s) * 3 + m) * 2 + piece], across,
        ).wait_recv()

    def settled(s, m, piece):
        at = halves[piece]
        far = part_at(wide_in, value_in, s, m, at)[...]
        return (acc[s, m, at] + far.astype(jnp.float32)).astype(jnp.bfloat16)

    def place(s, piece, of_core):
        which = side if piece == 0 else 1 - side
        first = (seqs[s] - core + of_core) * rows + which * block
        return pl.ds(pl.multiple_of(first, block), block)

    pieces = [(s, piece, m) for s in (OTHER, OWN) for piece in range(2) for m in (KEY, VALUE)]

    def number_of(s, piece, m):
        return (s * 2 + piece) * 2 + kinds[m]

    def kx_copy(s, piece, m):
        spot = cache.at[kinds[m], place(s, piece, core)]
        at = number_of(s, piece, m)
        return remote(spot, spot, kx_send.at[at], kx_recv.at[at], beside)

    def kd_copy(s, piece, m):
        spot = cache.at[kinds[m], place(s, piece, core)]
        at = number_of(s, piece, m)
        return remote(spot, spot, kd_send.at[at], kd_recv.at[at], partner)

    def settle(s, piece):
        for m in (KEY, VALUE):
            arrived(s, m, piece)
            fresh[kinds[m], s, halves[piece]] = settled(s, m, piece)

        @pl.when(grp == 0)
        def _():
            for m in (KEY, VALUE):
                cache[kinds[m], place(s, piece, core)] = settled(s, m, piece)
            for m in (KEY, VALUE):
                kx_copy(s, piece, m).start()
                kd_copy(s, piece, m).start()

    def relay(s, piece):
        @pl.when(grp != 0)
        def _():
            for m in (KEY, VALUE):
                kx_copy(s, piece, m).wait_recv()
                kd_copy(s, piece, m).start()

    take_z(1)
    for m in (KEY, VALUE):
        send(other, OTHER, halves[0], m)
        launch(partial(OTHER, m, 0))
    for m in (KEY, VALUE):
        keep(other, OTHER, halves[0], m)
    for far in range(2, planes - 1):
        take_z(far)
    settle(OTHER, 0)
    take_z(planes - 1)
    for m in (KEY, VALUE):
        send(other, OTHER, halves[1], m)
        launch(partial(OTHER, m, 1))
    for piece in range(2):
        send(other, OTHER, halves[piece], QUERY)
        launch(partial(OTHER, QUERY, piece))
    for m in (KEY, VALUE):
        keep(other, OTHER, halves[1], m)
    settle(OTHER, 1)
    keep(other, OTHER, everything, QUERY)
    relay(OTHER, 0)
    settle(OWN, 0)
    relay(OTHER, 1)
    settle(OWN, 1)
    for s in (OTHER, OWN):
        for piece in range(2):
            arrived(s, QUERY, piece)
            qbuf[s, halves[piece]] = settled(s, QUERY, piece)
    relay(OWN, 0)
    relay(OWN, 1)
    for s, piece, m in pieces:
        spot = cache.at[kinds[m], place(s, piece, 1 - core)]
        at = number_of(s, piece, m)
        remote(spot, spot, kd_send.at[at], kd_recv.at[at], partner).wait_recv()

    fresh_row = lax.broadcasted_iota(jnp.int32, (block, block), 0)
    fresh_col = lax.broadcasted_iota(jnp.int32, (block, block), 1)
    same = (
        lax.shift_right_logical(fresh_row, step_bits) == lax.shift_right_logical(fresh_col, step_bits)
    ) & (fresh_col <= fresh_row)
    fresh_bias = jnp.where(jnp.where(same, 1 - prompt_one, 0) == 1, 0.0, NEG)
    scale = HD ** (-0.5)

    def attend(s, piece, head):
        at = slice(piece * block, (piece + 1) * block)
        lanes = slice(head * HD, (head + 1) * HD)
        query = qbuf[s, at, lanes]

        def scored(key_block, mask):
            return lax.dot_general(
                query, key_block, contract_last, preferred_element_type=jnp.float32
            ) * scale + mask

        scores = [scored(cache[0, :, lanes], bias[s, at]), scored(fresh[0, s, at, lanes], fresh_bias)]
        values = [cache[1, :, lanes], fresh[1, s, at, lanes]]
        top = jnp.maximum(
            jnp.max(scores[0], axis=1, keepdims=True), jnp.max(scores[1], axis=1, keepdims=True)
        )
        total = jnp.zeros((block, 1), jnp.float32)
        summed = jnp.zeros((block, HD), jnp.float32)
        for score, value in zip(scores, values):
            weight = jnp.exp(score - top)
            total += jnp.sum(weight, axis=1, keepdims=True)
            summed += jnp.dot(weight.astype(jnp.bfloat16), value, preferred_element_type=jnp.float32)
        return (summed / total).astype(jnp.bfloat16)

    def out_copy(piece):
        return remote(osend.at[piece], orecv.at[piece], o_send.at[piece], o_recv.at[piece], across)

    for piece in range(2):
        for head in range(heads):
            osend[piece, :, head * HD : (head + 1) * HD] = attend(OTHER, piece, head)
        launch(out_copy(piece))
    for piece in range(2):
        for head in range(heads):
            lanes = pl.ds(pl.multiple_of(y * half + head * HD, HD), HD)
            out[piece * block : (piece + 1) * block, lanes] = attend(OWN, piece, head)
    for piece in range(2):
        out_copy(piece).wait_recv()
        out[piece * block : (piece + 1) * block, their_heads] = orecv[piece]

    for copy in sent:
        copy.wait_send()
    for step in pieces:
        kd_copy(*step).wait_send()
    for far in range(planes):
        for sub in range(SUBS):

            @pl.when((tp < planes - 1) & (tp >= far))
            def _():
                z_chunk(tp - far, sub, True).wait_send()

            @pl.when((tp > 0) & (tp + far < planes))
            def _():
                z_chunk(tp + far, sub, False).wait_send()

    @pl.when(grp == 0)
    def _():
        for step in pieces:
            kx_copy(*step).wait_send()


def fused(planes, hidden, w_query, w_key, w_value, prompt_len, page_table):
    rows, model = hidden.shape[1:]
    depth, width = w_query.shape
    half = width // 2
    block = rows // 2
    dma = pltpu.SemaphoreType.DMA
    anywhere = pl.BlockSpec(memory_space=pltpu.HBM)
    vmem = pl.BlockSpec(memory_space=pltpu.VMEM)
    result = pl.pallas_call(
        functools.partial(fused_kernel, planes),
        out_shape=jax.ShapeDtypeStruct((rows, width), jnp.bfloat16),
        in_specs=[anywhere] * 6,
        out_specs=vmem,
        scratch_shapes=[
            pltpu.VMEM((1, prompt_len.shape[0]), jnp.int32),
            pltpu.VMEM(page_table.shape[::-1], jnp.int32),
            pltpu.VMEM((rows, 2 * depth), jnp.bfloat16),
            pltpu.VMEM((rows, 2 * depth), jnp.bfloat16),
            pltpu.VMEM((3, 2 * depth, width), jnp.bfloat16),
            pltpu.VMEM((2, 3, rows, half), jnp.float32),
            pltpu.VMEM((2, 2, rows, half), jnp.float32),
            pltpu.VMEM((2, 2, rows, half), jnp.float32),
            pltpu.VMEM((2, rows, half), jnp.bfloat16),
            pltpu.VMEM((2, rows, half), jnp.bfloat16),
            pltpu.VMEM((2, rows, half), jnp.bfloat16),
            pltpu.VMEM((2, 2, rows, half), jnp.bfloat16),
            pltpu.VMEM((2, 4 * rows, half), jnp.bfloat16),
            pltpu.VMEM((2, rows, 4 * rows), jnp.float32),
            pltpu.VMEM((2, block, half), jnp.bfloat16),
            pltpu.VMEM((2, block, half), jnp.bfloat16),
            dma((6,)), dma((3,)), dma((3,)),
            dma((SUBS,)), dma((SUBS,)), dma((planes * SUBS,)), dma((planes * SUBS,)), dma((planes * SUBS,)),
            dma((12,)), dma((12,)),
            dma((8,)), dma((8,)), dma((8,)), dma((8,)),
            dma((2,)), dma((2,)),
        ],
        compiler_params=pltpu.CompilerParams(
            collective_id=0, has_side_effects=True, vmem_limit_bytes=67043328
        ),
    )(hidden, w_query, w_key, w_value, prompt_len.reshape(1, -1), page_table.T)
    return result[None]


def solution(mesh):
    planes = mesh.shape["tp"]
    paired = mesh.shape["grp"] == 2 and mesh.shape["seq"] == 4 and planes == 4
    return jax.shard_map(
        functools.partial(fused, planes) if paired else on_device,
        mesh=mesh,
        in_specs=(P("grp", "seq", None), P("seq", "tp"), P("seq", "tp"), P("seq", "tp"), P(), P()),
        out_specs=P("grp", "seq", "tp"),
        check_vma=False,
    )
```

```python
import functools
import math

import jax
import jax.numpy as jnp
from jax import lax
from jax.experimental import pallas as pl
from jax.experimental.pallas import tpu as pltpu
from jax.sharding import PartitionSpec as P

HD = 128
PAGE = 16
STEPS = 4


NEG = -1e30


def from_behind(value, axis, steps):
    count = lax.axis_size(axis)
    first, last = (max(0, -steps), min(count, count - steps))
    return lax.ppermute(value, axis, [(source, source + steps) for source in range(first, last)])


def partial_attention(query, keys, values, allowed):
    rows = query.shape[0]
    heads = query.shape[1] // HD
    query_heads = query.reshape(rows, heads, HD)
    key_heads = keys.reshape(keys.shape[0], heads, HD)
    value_heads = values.reshape(values.shape[0], heads, HD)
    scores = jnp.einsum(
        "rhd,shd->hrs", query_heads, key_heads, preferred_element_type=jnp.float32
    ) * HD ** (-0.5)
    scores = jnp.where(allowed[None], scores, NEG)
    top = jnp.max(scores, axis=2)
    weights = jnp.where(allowed[None], jnp.exp(scores - top[:, :, None]), 0.0)
    total = jnp.sum(weights, axis=2)
    summed = jnp.einsum(
        "hrs,shd->rhd",
        weights.astype(jnp.bfloat16),
        value_heads,
        preferred_element_type=jnp.float32,
    )
    return (top, total, summed.reshape(rows, heads * HD))


def rescale(summed, factor):
    rows = summed.shape[0]
    heads = factor.shape[0]
    return (summed.reshape(rows, heads, HD) * factor.T[:, :, None]).reshape(rows, heads * HD)


def combine(first, second):
    top = jnp.maximum(first[0], second[0])
    early = jnp.exp(first[0] - top)
    later = jnp.exp(second[0] - top)
    return (
        top,
        first[1] * early + second[1] * later,
        rescale(first[2], early) + rescale(second[2], later),
    )


def finish(state):
    return rescale(state[2], 1.0 / state[1]).astype(jnp.bfloat16)


def row_mask(tables, lengths, key_pos):
    pages = key_pos // PAGE
    member = jnp.any(tables[:, :, None] == pages[None, None, :], axis=1)
    allowed = member & (key_pos[None, :] < lengths[:, None])
    return jnp.repeat(allowed, STEPS, axis=0)


def blocked(carry, keys, values, query, mask_of):
    count = keys.shape[0]
    block = math.gcd(count, 512)

    def one_block(state, offset):
        piece_keys = lax.dynamic_slice_in_dim(keys, offset, block, 0)
        piece_values = lax.dynamic_slice_in_dim(values, offset, block, 0)
        key_pos = offset + jnp.arange(block)
        return (
            combine(state, partial_attention(query, piece_keys, piece_values, mask_of(key_pos))),
            None,
        )

    offsets = jnp.arange(count // block) * block
    state, unused = lax.scan(one_block, carry, offsets)
    return state


def on_device(hidden, w_query, w_key, w_value, prompt_len, page_table):
    local = hidden[0]
    rows = local.shape[0]
    width = w_query.shape[1]
    heads = width // HD
    seq_index = lax.axis_index("seq")
    is_prompt = lax.axis_index("grp") == 0
    empty = jnp.zeros((rows, width), jnp.float32)
    piece = (
        lax.all_gather(w_query, "seq", axis=0, tiled=True),
        lax.all_gather(w_key, "seq", axis=0, tiled=True),
        lax.all_gather(w_value, "seq", axis=0, tiled=True),
    )
    projected = tuple(
        (jnp.dot(local, weight, preferred_element_type=jnp.float32) for weight in piece)
    )
    query, keys, values = [item.astype(jnp.bfloat16) for item in projected]
    positions = seq_index * rows + jnp.arange(rows)
    start_state = (
        jnp.full((heads, rows), NEG, jnp.float32),
        jnp.zeros((heads, rows), jnp.float32),
        empty,
    )
    given_keys, given_values = from_behind((keys, values), "grp", 1)
    cache_keys = jnp.where(is_prompt, keys, given_keys)
    cache_values = jnp.where(is_prompt, values, given_values)
    row_count = rows // STEPS
    own_tables = lax.dynamic_slice_in_dim(page_table, seq_index * row_count, row_count, 0)
    own_lengths = lax.dynamic_slice_in_dim(prompt_len, seq_index * row_count, row_count, 0)

    def mask_of(key_pos):
        causal = key_pos[None, :] <= positions[:, None]
        listed = row_mask(own_tables, own_lengths, key_pos)
        return jnp.where(is_prompt, causal, listed)

    piece = (
        lax.all_gather(cache_keys, "seq", axis=0, tiled=True),
        lax.all_gather(cache_values, "seq", axis=0, tiled=True),
    )
    state = blocked(start_state, piece[0], piece[1], query, mask_of)
    frame_row = positions // STEPS
    own_rows = (frame_row[:, None] == frame_row[None, :]) & (
        positions[None, :] <= positions[:, None]
    )
    fresh = partial_attention(query, keys, values, own_rows)
    prefill_out = finish(state)
    decode_out = finish(combine(state, fresh))
    return jnp.where(is_prompt, prefill_out, decode_out)[None]


QUERY, KEY, VALUE = 0, 1, 2
OWN, OTHER = 0, 1
SUBS = 2


def fused_kernel(
    planes, hidden, w_query, w_key, w_value, lengths_in, tables_in, out,
    lengths, tables, own, other, weights, acc, wide_out, wide_in, value_out, value_in, qbuf, fresh, cache, bias, osend, orecv,
    local_sem, w_send, w_recv, hy_send, hy_recv, up_send, down_send, hz_recv, p_send, p_recv,
    kx_send, kx_recv, kd_send, kd_recv, o_send, o_recv,
):
    inputs = {QUERY: w_query, KEY: w_key, VALUE: w_value}
    rows = hidden.shape[1]
    depth, width = w_query.shape
    span = 2 * depth
    half = width // 2
    heads = half // HD
    block = rows // 2
    chunk = rows // planes // SUBS
    grp = lax.axis_index("grp")
    seq = lax.axis_index("seq")
    tp = lax.axis_index("tp")
    y = seq // 2
    core = seq % 2
    side = tp // (planes // 2)
    partner = {"seq": 2 * y + 1 - core}
    across = {"seq": 2 * (1 - y) + core}
    beside = {"grp": 1 - grp}
    above = {"tp": lax.rem(tp + 1, planes)}
    below = {"tp": lax.rem(tp + planes - 1, planes)}
    kinds = {KEY: 0, VALUE: 1}
    seqs = [2 * y + core, 2 * (1 - y) + core]
    my_heads = pl.ds(pl.multiple_of(y * half, half), half)
    their_heads = pl.ds(pl.multiple_of((1 - y) * half, half), half)
    plane_rows = rows // planes
    starts = (side * block, (planes // 2 - side) * plane_rows, (planes - 1) * (1 - side) * plane_rows)
    sizes = (block, plane_rows, plane_rows)
    parts = [pl.ds(pl.multiple_of(start, plane_rows), size) for start, size in zip(starts, sizes)]

    def remote(src, dst, send, recv, to):
        return pltpu.make_async_remote_copy(
            src_ref=src, dst_ref=dst, send_sem=send, recv_sem=recv,
            device_id=to, device_id_type=pl.DeviceIdType.MESH,
        )

    my_depth = pl.ds(pl.multiple_of(core * depth, depth), depth)
    keeps = {m: pltpu.make_async_copy(inputs[m], weights.at[m, my_depth], local_sem.at[m]) for m in inputs}
    table_keep = pltpu.make_async_copy(tables_in, tables, local_sem.at[3])
    length_keep = pltpu.make_async_copy(lengths_in, lengths, local_sem.at[4])
    own_keep = pltpu.make_async_copy(
        hidden.at[0, :, pl.ds(pl.multiple_of(y * span, span), span)], own, local_sem.at[5]
    )
    table_keep.start()
    length_keep.start()
    own_keep.start()
    for m in (KEY, VALUE, QUERY):
        keeps[m].start()

    barrier = pltpu.get_barrier_semaphore()
    for peer in (across, partner, beside):
        pl.semaphore_signal(barrier, inc=1, device_id=peer, device_id_type=pl.DeviceIdType.MESH)

    @pl.when(tp < planes - 1)
    def _():
        pl.semaphore_signal(barrier, inc=1, device_id=above, device_id_type=pl.DeviceIdType.MESH)

    @pl.when(tp > 0)
    def _():
        pl.semaphore_signal(barrier, inc=1, device_id=below, device_id_type=pl.DeviceIdType.MESH)

    ends = jnp.where(tp == 0, 1, 0) + jnp.where(tp == planes - 1, 1, 0)
    pl.semaphore_wait(barrier, 5 - ends)

    def chunk_rows(plane, sub):
        return pl.ds(pl.multiple_of((plane * SUBS + sub) * chunk, chunk), chunk)

    def y_chunk(sub):
        take = chunk_rows(tp, sub)
        return remote(
            hidden.at[0, take, pl.ds(pl.multiple_of((1 - y) * span, span), span)], other.at[take],
            hy_send.at[sub], hy_recv.at[sub], across,
        )

    def z_chunk(plane, sub, up):
        take = chunk_rows(plane, sub)
        at = plane * SUBS + sub
        return remote(
            other.at[take], other.at[take], (up_send if up else down_send).at[at], hz_recv.at[at],
            above if up else below,
        )

    sent = []

    def launch(copy):
        copy.start()
        sent.append(copy)

    for sub in range(SUBS):
        launch(y_chunk(sub))
    swaps = {
        m: remote(inputs[m], weights.at[m, my_depth], w_send.at[m], w_recv.at[m], partner) for m in inputs
    }
    for m in (KEY, VALUE, QUERY):
        launch(swaps[m])

    table_keep.wait()
    length_keep.wait()
    total_rows = tables.shape[1]
    keys = cache.shape[1]
    pages = keys // PAGE
    decode_rows = rows // STEPS
    step_bits = STEPS.bit_length() - 1
    page_bits = PAGE.bit_length() - 1
    prompt_one = jnp.where(grp == 0, 1, 0)
    contract_last = (((1,), (1,)), ((), ()))
    table = tables[...]
    page_row = lax.broadcasted_iota(jnp.int32, (pages, total_rows), 0)
    member = table[0:1, :] == page_row
    for listed in range(1, table.shape[0]):
        member = member | (table[listed : listed + 1, :] == page_row)
    member = jnp.where(member, 1.0, 0.0).astype(jnp.bfloat16)
    unfold = lax.broadcasted_iota(jnp.int32, (keys, pages), 1) == lax.shift_right_logical(
        lax.broadcasted_iota(jnp.int32, (keys, pages), 0), page_bits
    )
    unfold = jnp.where(unfold, 1.0, 0.0).astype(jnp.bfloat16)
    seen = jnp.dot(unfold, member, preferred_element_type=jnp.float32)
    key_pos = lax.broadcasted_iota(jnp.int32, (keys, total_rows), 0)
    seen = jnp.where(key_pos < lengths[...], seen, 0.0).astype(jnp.bfloat16)
    for s in (OWN, OTHER):
        spread = (
            lax.shift_right_logical(lax.broadcasted_iota(jnp.int32, (rows, total_rows), 0), step_bits)
            + seqs[s] * decode_rows
            == lax.broadcasted_iota(jnp.int32, (rows, total_rows), 1)
        )
        spread = jnp.where(spread, 1.0, 0.0).astype(jnp.bfloat16)
        listed = lax.dot_general(spread, seen, contract_last, preferred_element_type=jnp.float32)
        causal = (
            lax.broadcasted_iota(jnp.int32, (rows, keys), 1)
            <= lax.broadcasted_iota(jnp.int32, (rows, keys), 0) + seqs[s] * rows
        )
        allowed = jnp.where(prompt_one == 1, jnp.where(causal, 1.0, 0.0), listed)
        bias[s] = jnp.where(allowed > 0.5, 0.0, NEG)

    def project(source, at, m, lanes):
        return jnp.dot(source[at, :], weights[m, :, lanes], preferred_element_type=jnp.float32)

    def part_at(wide, narrow, s, m, at):
        return narrow.at[s, at] if m == VALUE else wide.at[s, m, at]

    def send(source, s, at, m):
        spot = part_at(wide_out, value_out, s, m, at)
        spot[...] = project(source, at, m, their_heads).astype(spot.dtype)

    def keep(source, s, at, m):
        acc[s, m, at] = project(source, at, m, my_heads)

    def both(source, s, at, m):
        send(source, s, at, m)
        keep(source, s, at, m)

    def partial(s, m, piece):
        at = parts[piece]
        number = (s * 3 + m) * 3 + piece
        return remote(
            part_at(wide_out, value_out, s, m, at), part_at(wide_in, value_in, 1 - s, m, at),
            p_send.at[number], p_recv.at[number], across,
        )

    everything = pl.ds(0, rows)

    def pass_on(plane, sub, up, down):
        if up:

            @pl.when(tp < planes - 1)
            def _():
                z_chunk(plane, sub, True).start()

        if down:

            @pl.when(tp > 0)
            def _():
                z_chunk(plane, sub, False).start()

    def take_y(sub):
        y_chunk(sub).wait_recv()
        pass_on(tp, sub, True, True)

    def take_z(far):
        for sub in range(SUBS):

            @pl.when(tp + far < planes)
            def _():
                z_chunk(tp + far, sub, False).wait_recv()
                pass_on(tp + far, sub, False, True)

            @pl.when(tp >= far)
            def _():
                z_chunk(tp - far, sub, True).wait_recv()
                pass_on(tp - far, sub, True, False)

    own_keep.wait()
    for at, m in enumerate((KEY, VALUE, QUERY)):
        keeps[m].wait()
        swaps[m].wait_recv()
        if at < SUBS:
            take_y(at)
        for piece in range(3):
            send(own, OWN, parts[piece], m)
            if m != QUERY:
                launch(partial(OWN, m, piece))
        keep(own, OWN, everything, m)
    for sub in range(3, SUBS):
        take_y(sub)

    def arrived(s, m, piece):
        at = parts[piece]
        remote(
            part_at(wide_out, value_out, s, m, at), part_at(wide_in, value_in, s, m, at),
            p_send.at[((1 - s) * 3 + m) * 3 + piece], p_recv.at[((1 - s) * 3 + m) * 3 + piece], across,
        ).wait_recv()

    def settled(s, m, piece):
        at = parts[piece]
        far = part_at(wide_in, value_in, s, m, at)[...]
        return (acc[s, m, at] + far.astype(jnp.float32)).astype(jnp.bfloat16)

    def place(s, piece, of_core):
        first = (seqs[s] - core + of_core) * rows + starts[piece]
        return pl.ds(pl.multiple_of(first, plane_rows), sizes[piece])

    pieces = [(s, piece, m) for s in (OTHER, OWN) for piece in range(3) for m in (KEY, VALUE)]

    def number_of(s, piece, m):
        return (s * 3 + piece) * 2 + kinds[m]

    def kx_copy(s, piece, m):
        spot = cache.at[kinds[m], place(s, piece, core)]
        at = number_of(s, piece, m)
        return remote(spot, spot, kx_send.at[at], kx_recv.at[at], beside)

    def kd_copy(s, piece, m):
        spot = cache.at[kinds[m], place(s, piece, core)]
        at = number_of(s, piece, m)
        return remote(spot, spot, kd_send.at[at], kd_recv.at[at], partner)

    def settle(s, piece):
        for m in (KEY, VALUE):
            arrived(s, m, piece)
            fresh[kinds[m], s, parts[piece]] = settled(s, m, piece)

        @pl.when(grp == 0)
        def _():
            for m in (KEY, VALUE):
                cache[kinds[m], place(s, piece, core)] = settled(s, m, piece)
            for m in (KEY, VALUE):
                kx_copy(s, piece, m).start()
                kd_copy(s, piece, m).start()

    def relay(s, piece):
        @pl.when(grp != 0)
        def _():
            for m in (KEY, VALUE):
                kx_copy(s, piece, m).wait_recv()
                kd_copy(s, piece, m).start()

    def others(piece):
        for m in (KEY, VALUE):
            send(other, OTHER, parts[piece], m)
            launch(partial(OTHER, m, piece))
        for m in (KEY, VALUE):
            keep(other, OTHER, parts[piece], m)

    def take_query(s):
        for piece in range(3):
            arrived(s, QUERY, piece)
            qbuf[s, parts[piece]] = settled(s, QUERY, piece)

    take_z(1)
    others(0)
    take_z(2)
    others(1)
    launch(partial(OWN, QUERY, 0))
    settle(OTHER, 0)
    settle(OTHER, 1)
    settle(OWN, 0)
    relay(OTHER, 0)
    take_z(3)
    others(2)
    for piece in (1, 2):
        launch(partial(OWN, QUERY, piece))
    for piece in range(3):
        send(other, OTHER, parts[piece], QUERY)
        launch(partial(OTHER, QUERY, piece))
    settle(OTHER, 2)
    relay(OTHER, 1)
    settle(OWN, 1)
    keep(other, OTHER, everything, QUERY)
    relay(OTHER, 2)
    relay(OWN, 0)
    settle(OWN, 2)
    relay(OWN, 1)
    take_query(OTHER)
    relay(OWN, 2)
    for s, piece, m in pieces:
        spot = cache.at[kinds[m], place(s, piece, 1 - core)]
        at = number_of(s, piece, m)
        remote(spot, spot, kd_send.at[at], kd_recv.at[at], partner).wait_recv()

    fresh_row = lax.broadcasted_iota(jnp.int32, (block, block), 0)
    fresh_col = lax.broadcasted_iota(jnp.int32, (block, block), 1)
    same = (
        lax.shift_right_logical(fresh_row, step_bits) == lax.shift_right_logical(fresh_col, step_bits)
    ) & (fresh_col <= fresh_row)
    fresh_bias = jnp.where(jnp.where(same, 1 - prompt_one, 0) == 1, 0.0, NEG)
    scale = HD ** (-0.5)

    def attend(s, piece, head):
        at = slice(piece * block, (piece + 1) * block)
        lanes = slice(head * HD, (head + 1) * HD)
        query = qbuf[s, at, lanes]

        def scored(key_block, mask):
            return lax.dot_general(
                query, key_block, contract_last, preferred_element_type=jnp.float32
            ) * scale + mask

        scores = [scored(cache[0, :, lanes], bias[s, at]), scored(fresh[0, s, at, lanes], fresh_bias)]
        values = [cache[1, :, lanes], fresh[1, s, at, lanes]]
        top = jnp.maximum(
            jnp.max(scores[0], axis=1, keepdims=True), jnp.max(scores[1], axis=1, keepdims=True)
        )
        total = jnp.zeros((block, 1), jnp.float32)
        summed = jnp.zeros((block, HD), jnp.float32)
        for score, value in zip(scores, values):
            weight = jnp.exp(score - top)
            total += jnp.sum(weight, axis=1, keepdims=True)
            summed += jnp.dot(weight.astype(jnp.bfloat16), value, preferred_element_type=jnp.float32)
        return (summed / total).astype(jnp.bfloat16)

    def out_copy(piece):
        return remote(osend.at[piece], orecv.at[piece], o_send.at[piece], o_recv.at[piece], across)

    for piece in range(2):
        for head in range(heads):
            osend[piece, :, head * HD : (head + 1) * HD] = attend(OTHER, piece, head)
        launch(out_copy(piece))
    take_query(OWN)
    for piece in range(2):
        for head in range(heads):
            lanes = pl.ds(pl.multiple_of(y * half + head * HD, HD), HD)
            out[piece * block : (piece + 1) * block, lanes] = attend(OWN, piece, head)
    for piece in range(2):
        out_copy(piece).wait_recv()
        out[piece * block : (piece + 1) * block, their_heads] = orecv[piece]

    for copy in sent:
        copy.wait_send()
    for step in pieces:
        kd_copy(*step).wait_send()
    for far in range(planes):
        for sub in range(SUBS):

            @pl.when((tp < planes - 1) & (tp >= far))
            def _():
                z_chunk(tp - far, sub, True).wait_send()

            @pl.when((tp > 0) & (tp + far < planes))
            def _():
                z_chunk(tp + far, sub, False).wait_send()

    @pl.when(grp == 0)
    def _():
        for step in pieces:
            kx_copy(*step).wait_send()


def fused(planes, hidden, w_query, w_key, w_value, prompt_len, page_table):
    rows, model = hidden.shape[1:]
    depth, width = w_query.shape
    half = width // 2
    block = rows // 2
    dma = pltpu.SemaphoreType.DMA
    anywhere = pl.BlockSpec(memory_space=pltpu.HBM)
    vmem = pl.BlockSpec(memory_space=pltpu.VMEM)
    result = pl.pallas_call(
        functools.partial(fused_kernel, planes),
        out_shape=jax.ShapeDtypeStruct((rows, width), jnp.bfloat16),
        in_specs=[anywhere] * 6,
        out_specs=vmem,
        scratch_shapes=[
            pltpu.VMEM((1, prompt_len.shape[0]), jnp.int32),
            pltpu.VMEM(page_table.shape[::-1], jnp.int32),
            pltpu.VMEM((rows, 2 * depth), jnp.bfloat16),
            pltpu.VMEM((rows, 2 * depth), jnp.bfloat16),
            pltpu.VMEM((3, 2 * depth, width), jnp.bfloat16),
            pltpu.VMEM((2, 3, rows, half), jnp.float32),
            pltpu.VMEM((2, 2, rows, half), jnp.float32),
            pltpu.VMEM((2, 2, rows, half), jnp.float32),
            pltpu.VMEM((2, rows, half), jnp.bfloat16),
            pltpu.VMEM((2, rows, half), jnp.bfloat16),
            pltpu.VMEM((2, rows, half), jnp.bfloat16),
            pltpu.VMEM((2, 2, rows, half), jnp.bfloat16),
            pltpu.VMEM((2, 4 * rows, half), jnp.bfloat16),
            pltpu.VMEM((2, rows, 4 * rows), jnp.float32),
            pltpu.VMEM((2, block, half), jnp.bfloat16),
            pltpu.VMEM((2, block, half), jnp.bfloat16),
            dma((6,)), dma((3,)), dma((3,)),
            dma((SUBS,)), dma((SUBS,)), dma((planes * SUBS,)), dma((planes * SUBS,)), dma((planes * SUBS,)),
            dma((18,)), dma((18,)),
            dma((12,)), dma((12,)), dma((12,)), dma((12,)),
            dma((2,)), dma((2,)),
        ],
        compiler_params=pltpu.CompilerParams(
            collective_id=0, has_side_effects=True, vmem_limit_bytes=67043328
        ),
    )(hidden, w_query, w_key, w_value, prompt_len.reshape(1, -1), page_table.T)
    return result[None]


def solution(mesh):
    planes = mesh.shape["tp"]
    paired = mesh.shape["grp"] == 2 and mesh.shape["seq"] == 4 and planes == 4
    return jax.shard_map(
        functools.partial(fused, planes) if paired else on_device,
        mesh=mesh,
        in_specs=(P("grp", "seq", None), P("seq", "tp"), P("seq", "tp"), P("seq", "tp"), P(), P()),
        out_specs=P("grp", "seq", "tp"),
        check_vma=False,
    )
```

```python
import functools
import math

import jax
import jax.numpy as jnp
from jax import lax
from jax.experimental import pallas as pl
from jax.experimental.pallas import tpu as pltpu
from jax.sharding import PartitionSpec as P

HD = 128
PAGE = 16
STEPS = 4


NEG = -1e30


def from_behind(value, axis, steps):
    count = lax.axis_size(axis)
    first, last = (max(0, -steps), min(count, count - steps))
    return lax.ppermute(value, axis, [(source, source + steps) for source in range(first, last)])


def partial_attention(query, keys, values, allowed):
    rows = query.shape[0]
    heads = query.shape[1] // HD
    query_heads = query.reshape(rows, heads, HD)
    key_heads = keys.reshape(keys.shape[0], heads, HD)
    value_heads = values.reshape(values.shape[0], heads, HD)
    scores = jnp.einsum(
        "rhd,shd->hrs", query_heads, key_heads, preferred_element_type=jnp.float32
    ) * HD ** (-0.5)
    scores = jnp.where(allowed[None], scores, NEG)
    top = jnp.max(scores, axis=2)
    weights = jnp.where(allowed[None], jnp.exp(scores - top[:, :, None]), 0.0)
    total = jnp.sum(weights, axis=2)
    summed = jnp.einsum(
        "hrs,shd->rhd",
        weights.astype(jnp.bfloat16),
        value_heads,
        preferred_element_type=jnp.float32,
    )
    return (top, total, summed.reshape(rows, heads * HD))


def rescale(summed, factor):
    rows = summed.shape[0]
    heads = factor.shape[0]
    return (summed.reshape(rows, heads, HD) * factor.T[:, :, None]).reshape(rows, heads * HD)


def combine(first, second):
    top = jnp.maximum(first[0], second[0])
    early = jnp.exp(first[0] - top)
    later = jnp.exp(second[0] - top)
    return (
        top,
        first[1] * early + second[1] * later,
        rescale(first[2], early) + rescale(second[2], later),
    )


def finish(state):
    return rescale(state[2], 1.0 / state[1]).astype(jnp.bfloat16)


def row_mask(tables, lengths, key_pos):
    pages = key_pos // PAGE
    member = jnp.any(tables[:, :, None] == pages[None, None, :], axis=1)
    allowed = member & (key_pos[None, :] < lengths[:, None])
    return jnp.repeat(allowed, STEPS, axis=0)


def blocked(carry, keys, values, query, mask_of):
    count = keys.shape[0]
    block = math.gcd(count, 512)

    def one_block(state, offset):
        piece_keys = lax.dynamic_slice_in_dim(keys, offset, block, 0)
        piece_values = lax.dynamic_slice_in_dim(values, offset, block, 0)
        key_pos = offset + jnp.arange(block)
        return (
            combine(state, partial_attention(query, piece_keys, piece_values, mask_of(key_pos))),
            None,
        )

    offsets = jnp.arange(count // block) * block
    state, unused = lax.scan(one_block, carry, offsets)
    return state


def on_device(hidden, w_query, w_key, w_value, prompt_len, page_table):
    local = hidden[0]
    rows = local.shape[0]
    width = w_query.shape[1]
    heads = width // HD
    seq_index = lax.axis_index("seq")
    is_prompt = lax.axis_index("grp") == 0
    empty = jnp.zeros((rows, width), jnp.float32)
    piece = (
        lax.all_gather(w_query, "seq", axis=0, tiled=True),
        lax.all_gather(w_key, "seq", axis=0, tiled=True),
        lax.all_gather(w_value, "seq", axis=0, tiled=True),
    )
    projected = tuple(
        (jnp.dot(local, weight, preferred_element_type=jnp.float32) for weight in piece)
    )
    query, keys, values = [item.astype(jnp.bfloat16) for item in projected]
    positions = seq_index * rows + jnp.arange(rows)
    start_state = (
        jnp.full((heads, rows), NEG, jnp.float32),
        jnp.zeros((heads, rows), jnp.float32),
        empty,
    )
    given_keys, given_values = from_behind((keys, values), "grp", 1)
    cache_keys = jnp.where(is_prompt, keys, given_keys)
    cache_values = jnp.where(is_prompt, values, given_values)
    row_count = rows // STEPS
    own_tables = lax.dynamic_slice_in_dim(page_table, seq_index * row_count, row_count, 0)
    own_lengths = lax.dynamic_slice_in_dim(prompt_len, seq_index * row_count, row_count, 0)

    def mask_of(key_pos):
        causal = key_pos[None, :] <= positions[:, None]
        listed = row_mask(own_tables, own_lengths, key_pos)
        return jnp.where(is_prompt, causal, listed)

    piece = (
        lax.all_gather(cache_keys, "seq", axis=0, tiled=True),
        lax.all_gather(cache_values, "seq", axis=0, tiled=True),
    )
    state = blocked(start_state, piece[0], piece[1], query, mask_of)
    frame_row = positions // STEPS
    own_rows = (frame_row[:, None] == frame_row[None, :]) & (
        positions[None, :] <= positions[:, None]
    )
    fresh = partial_attention(query, keys, values, own_rows)
    prefill_out = finish(state)
    decode_out = finish(combine(state, fresh))
    return jnp.where(is_prompt, prefill_out, decode_out)[None]


QUERY, KEY, VALUE = 0, 1, 2
OWN, OTHER = 0, 1
SUBS = 2


def fused_kernel(
    planes, hidden, w_query, w_key, w_value, lengths_in, tables_in, out,
    lengths, tables, stage, own, other, weights, acc, wide_out, wide_in, value_out, value_in, qbuf, fresh, cache, bias, osend, oself,
    local_sem, w_send, w_recv, hy_send, hy_recv, up_send, down_send, hz_recv, p_send, p_recv,
    kx_send, kx_recv, kd_send, kd_recv, o_send, o_recv, o_keep,
):
    inputs = {QUERY: w_query, KEY: w_key, VALUE: w_value}
    rows = hidden.shape[1]
    depth, width = w_query.shape
    span = 2 * depth
    half = width // 2
    heads = half // HD
    block = rows // 2
    chunk = rows // planes // SUBS
    grp = lax.axis_index("grp")
    seq = lax.axis_index("seq")
    tp = lax.axis_index("tp")
    y = seq // 2
    core = seq % 2
    side = tp // (planes // 2)
    partner = {"seq": 2 * y + 1 - core}
    across = {"seq": 2 * (1 - y) + core}
    beside = {"grp": 1 - grp}
    above = {"tp": lax.rem(tp + 1, planes)}
    below = {"tp": lax.rem(tp + planes - 1, planes)}
    kinds = {KEY: 0, VALUE: 1}
    seqs = [2 * y + core, 2 * (1 - y) + core]
    my_heads = pl.ds(pl.multiple_of(y * half, half), half)
    their_heads = pl.ds(pl.multiple_of((1 - y) * half, half), half)
    plane_rows = rows // planes
    starts = (side * block, (planes // 2 - side) * plane_rows, (planes - 1) * (1 - side) * plane_rows)
    sizes = (block, plane_rows, plane_rows)
    parts = [pl.ds(pl.multiple_of(start, plane_rows), size) for start, size in zip(starts, sizes)]

    def remote(src, dst, send, recv, to):
        return pltpu.make_async_remote_copy(
            src_ref=src, dst_ref=dst, send_sem=send, recv_sem=recv,
            device_id=to, device_id_type=pl.DeviceIdType.MESH,
        )

    my_depth = pl.ds(pl.multiple_of(core * depth, depth), depth)
    keeps = {m: pltpu.make_async_copy(inputs[m], weights.at[m, my_depth], local_sem.at[m]) for m in inputs}
    table_keep = pltpu.make_async_copy(tables_in, tables, local_sem.at[3])
    length_keep = pltpu.make_async_copy(lengths_in, lengths, local_sem.at[4])
    own_keep = pltpu.make_async_copy(
        hidden.at[0, :, pl.ds(pl.multiple_of(y * span, span), span)], own, local_sem.at[5]
    )
    def staged(sub):
        take = pl.ds(pl.multiple_of((tp * SUBS + sub) * chunk, chunk), chunk)
        return pltpu.make_async_copy(
            hidden.at[0, take, pl.ds(pl.multiple_of((1 - y) * span, span), span)], stage.at[sub],
            local_sem.at[6 + sub],
        )

    barrier = pltpu.get_barrier_semaphore()
    for peer in (across, partner, beside):
        pl.semaphore_signal(barrier, inc=1, device_id=peer, device_id_type=pl.DeviceIdType.MESH)

    @pl.when(tp < planes - 1)
    def _():
        pl.semaphore_signal(barrier, inc=1, device_id=above, device_id_type=pl.DeviceIdType.MESH)

    @pl.when(tp > 0)
    def _():
        pl.semaphore_signal(barrier, inc=1, device_id=below, device_id_type=pl.DeviceIdType.MESH)

    for sub in range(SUBS):
        staged(sub).start()
    for m in (KEY, VALUE, QUERY):
        keeps[m].start()
    own_keep.start()
    table_keep.start()
    length_keep.start()
    ends = jnp.where(tp == 0, 1, 0) + jnp.where(tp == planes - 1, 1, 0)
    pl.semaphore_wait(barrier, 5 - ends)

    def chunk_rows(plane, sub):
        return pl.ds(pl.multiple_of((plane * SUBS + sub) * chunk, chunk), chunk)

    def y_chunk(sub):
        take = chunk_rows(tp, sub)
        return remote(
            stage.at[sub], other.at[take],
            hy_send.at[sub], hy_recv.at[sub], across,
        )

    def z_chunk(plane, sub, up):
        take = chunk_rows(plane, sub)
        at = plane * SUBS + sub
        return remote(
            other.at[take], other.at[take], (up_send if up else down_send).at[at], hz_recv.at[at],
            above if up else below,
        )

    sent = []

    def launch(copy):
        copy.start()
        sent.append(copy)

    for sub in range(SUBS):
        staged(sub).wait()
        launch(y_chunk(sub))
    swaps = {
        m: remote(weights.at[m, my_depth], weights.at[m, my_depth], w_send.at[m], w_recv.at[m], partner) for m in inputs
    }
    for m in (KEY, VALUE, QUERY):
        keeps[m].wait()
        launch(swaps[m])

    table_keep.wait()
    length_keep.wait()
    total_rows = tables.shape[1]
    keys = cache.shape[1]
    pages = keys // PAGE
    decode_rows = rows // STEPS
    step_bits = STEPS.bit_length() - 1
    page_bits = PAGE.bit_length() - 1
    prompt_one = jnp.where(grp == 0, 1, 0)
    contract_last = (((1,), (1,)), ((), ()))
    table = tables[...]
    page_row = lax.broadcasted_iota(jnp.int32, (pages, total_rows), 0)
    member = table[0:1, :] == page_row
    for listed in range(1, table.shape[0]):
        member = member | (table[listed : listed + 1, :] == page_row)
    member = jnp.where(member, 1.0, 0.0).astype(jnp.bfloat16)
    unfold = lax.broadcasted_iota(jnp.int32, (keys, pages), 1) == lax.shift_right_logical(
        lax.broadcasted_iota(jnp.int32, (keys, pages), 0), page_bits
    )
    unfold = jnp.where(unfold, 1.0, 0.0).astype(jnp.bfloat16)
    seen = jnp.dot(unfold, member, preferred_element_type=jnp.float32)
    key_pos = lax.broadcasted_iota(jnp.int32, (keys, total_rows), 0)
    seen = jnp.where(key_pos < lengths[...], seen, 0.0).astype(jnp.bfloat16)
    for s in (OWN, OTHER):
        spread = (
            lax.shift_right_logical(lax.broadcasted_iota(jnp.int32, (rows, total_rows), 0), step_bits)
            + seqs[s] * decode_rows
            == lax.broadcasted_iota(jnp.int32, (rows, total_rows), 1)
        )
        spread = jnp.where(spread, 1.0, 0.0).astype(jnp.bfloat16)
        listed = lax.dot_general(spread, seen, contract_last, preferred_element_type=jnp.float32)
        causal = (
            lax.broadcasted_iota(jnp.int32, (rows, keys), 1)
            <= lax.broadcasted_iota(jnp.int32, (rows, keys), 0) + seqs[s] * rows
        )
        allowed = jnp.where(prompt_one == 1, jnp.where(causal, 1.0, 0.0), listed)
        bias[s] = jnp.where(allowed > 0.5, 0.0, NEG)

    def project(source, at, m, lanes):
        return jnp.dot(source[at, :], weights[m, :, lanes], preferred_element_type=jnp.float32)

    def part_at(wide, narrow, s, m, at):
        return narrow.at[s, at] if m == VALUE else wide.at[s, m, at]

    def send(source, s, at, m):
        spot = part_at(wide_out, value_out, s, m, at)
        spot[...] = project(source, at, m, their_heads).astype(spot.dtype)

    def keep(source, s, at, m):
        acc[s, m, at] = project(source, at, m, my_heads)

    def both(source, s, at, m):
        send(source, s, at, m)
        keep(source, s, at, m)

    def partial(s, m, piece):
        at = parts[piece]
        number = (s * 3 + m) * 3 + piece
        return remote(
            part_at(wide_out, value_out, s, m, at), part_at(wide_in, value_in, 1 - s, m, at),
            p_send.at[number], p_recv.at[number], across,
        )

    everything = pl.ds(0, rows)

    def pass_on(plane, sub, up, down):
        if up:

            @pl.when(tp < planes - 1)
            def _():
                z_chunk(plane, sub, True).start()

        if down:

            @pl.when(tp > 0)
            def _():
                z_chunk(plane, sub, False).start()

    def take_y(sub):
        y_chunk(sub).wait_recv()
        pass_on(tp, sub, True, True)

    def take_z(far):
        for sub in range(SUBS):

            @pl.when(tp + far < planes)
            def _():
                z_chunk(tp + far, sub, False).wait_recv()
                pass_on(tp + far, sub, False, True)

            @pl.when(tp >= far)
            def _():
                z_chunk(tp - far, sub, True).wait_recv()
                pass_on(tp - far, sub, True, False)

    own_keep.wait()
    for at, m in enumerate((KEY, VALUE, QUERY)):
        swaps[m].wait_recv()
        if at < SUBS:
            take_y(at)
        for piece in range(3):
            send(own, OWN, parts[piece], m)
            if m != QUERY:
                launch(partial(OWN, m, piece))
        keep(own, OWN, everything, m)
    for sub in range(3, SUBS):
        take_y(sub)

    def arrived(s, m, piece):
        at = parts[piece]
        remote(
            part_at(wide_out, value_out, s, m, at), part_at(wide_in, value_in, s, m, at),
            p_send.at[((1 - s) * 3 + m) * 3 + piece], p_recv.at[((1 - s) * 3 + m) * 3 + piece], across,
        ).wait_recv()

    def settled(s, m, piece):
        at = parts[piece]
        far = part_at(wide_in, value_in, s, m, at)[...]
        return (acc[s, m, at] + far.astype(jnp.float32)).astype(jnp.bfloat16)

    def place(s, piece, of_core):
        first = (seqs[s] - core + of_core) * rows + starts[piece]
        return pl.ds(pl.multiple_of(first, plane_rows), sizes[piece])

    pieces = [(s, piece, m) for s in (OTHER, OWN) for piece in range(3) for m in (KEY, VALUE)]

    def number_of(s, piece, m):
        return (s * 3 + piece) * 2 + kinds[m]

    def kx_copy(s, piece, m):
        spot = cache.at[kinds[m], place(s, piece, core)]
        at = number_of(s, piece, m)
        return remote(spot, spot, kx_send.at[at], kx_recv.at[at], beside)

    def kd_copy(s, piece, m):
        spot = cache.at[kinds[m], place(s, piece, core)]
        at = number_of(s, piece, m)
        return remote(spot, spot, kd_send.at[at], kd_recv.at[at], partner)

    def settle(s, piece):
        for m in (KEY, VALUE):
            arrived(s, m, piece)
            fresh[kinds[m], s, parts[piece]] = settled(s, m, piece)

        @pl.when(grp == 0)
        def _():
            for m in (KEY, VALUE):
                cache[kinds[m], place(s, piece, core)] = settled(s, m, piece)
            for m in (KEY, VALUE):
                kx_copy(s, piece, m).start()
                kd_copy(s, piece, m).start()

    def relay(s, piece):
        @pl.when(grp != 0)
        def _():
            for m in (KEY, VALUE):
                kx_copy(s, piece, m).wait_recv()
                kd_copy(s, piece, m).start()

    def others(piece):
        for m in (KEY, VALUE):
            send(other, OTHER, parts[piece], m)
            launch(partial(OTHER, m, piece))
        for m in (KEY, VALUE):
            keep(other, OTHER, parts[piece], m)

    def take_query(s):
        for piece in range(3):
            arrived(s, QUERY, piece)
            qbuf[s, parts[piece]] = settled(s, QUERY, piece)

    take_z(1)
    others(0)
    take_z(2)
    others(1)
    launch(partial(OWN, QUERY, 0))
    settle(OTHER, 0)
    settle(OTHER, 1)
    settle(OWN, 0)
    relay(OTHER, 0)
    take_z(3)
    others(2)
    for piece in (1, 2):
        launch(partial(OWN, QUERY, piece))
    for piece in range(3):
        send(other, OTHER, parts[piece], QUERY)
        launch(partial(OTHER, QUERY, piece))
    settle(OTHER, 2)
    relay(OTHER, 1)
    settle(OWN, 1)
    keep(other, OTHER, everything, QUERY)
    relay(OTHER, 2)
    relay(OWN, 0)
    settle(OWN, 2)
    relay(OWN, 1)
    take_query(OTHER)
    relay(OWN, 2)
    for s, piece, m in pieces:
        spot = cache.at[kinds[m], place(s, piece, 1 - core)]
        at = number_of(s, piece, m)
        remote(spot, spot, kd_send.at[at], kd_recv.at[at], partner).wait_recv()

    fresh_row = lax.broadcasted_iota(jnp.int32, (block, block), 0)
    fresh_col = lax.broadcasted_iota(jnp.int32, (block, block), 1)
    same = (
        lax.shift_right_logical(fresh_row, step_bits) == lax.shift_right_logical(fresh_col, step_bits)
    ) & (fresh_col <= fresh_row)
    fresh_bias = jnp.where(jnp.where(same, 1 - prompt_one, 0) == 1, 0.0, NEG)
    scale = HD ** (-0.5)

    def attend(s, piece, head):
        at = slice(piece * block, (piece + 1) * block)
        lanes = slice(head * HD, (head + 1) * HD)
        query = qbuf[s, at, lanes]

        def scored(key_block, mask):
            return lax.dot_general(
                query, key_block, contract_last, preferred_element_type=jnp.float32
            ) * scale + mask

        scores = [scored(cache[0, :, lanes], bias[s, at]), scored(fresh[0, s, at, lanes], fresh_bias)]
        values = [cache[1, :, lanes], fresh[1, s, at, lanes]]
        top = jnp.maximum(
            jnp.max(scores[0], axis=1, keepdims=True), jnp.max(scores[1], axis=1, keepdims=True)
        )
        total = jnp.zeros((block, 1), jnp.float32)
        summed = jnp.zeros((block, HD), jnp.float32)
        for score, value in zip(scores, values):
            weight = jnp.exp(score - top)
            total += jnp.sum(weight, axis=1, keepdims=True)
            summed += jnp.dot(weight.astype(jnp.bfloat16), value, preferred_element_type=jnp.float32)
        return (summed / total).astype(jnp.bfloat16)

    def out_copy(piece):
        span = pl.ds(piece * block, block)
        return remote(osend.at[piece], out.at[span, my_heads], o_send.at[piece], o_recv.at[piece], across)

    def out_keep(piece):
        span = pl.ds(piece * block, block)
        return pltpu.make_async_copy(oself.at[piece], out.at[span, my_heads], o_keep.at[piece])

    for piece in range(2):
        for head in range(heads):
            osend[piece, :, head * HD : (head + 1) * HD] = attend(OTHER, piece, head)
        launch(out_copy(piece))
    take_query(OWN)
    for piece in range(2):
        for head in range(heads):
            oself[piece, :, head * HD : (head + 1) * HD] = attend(OWN, piece, head)
        out_keep(piece).start()
    for piece in range(2):
        span = pl.ds(piece * block, block)
        remote(osend.at[piece], out.at[span, their_heads], o_send.at[piece], o_recv.at[piece], across).wait_recv()
        out_keep(piece).wait()

    for copy in sent:
        copy.wait_send()
    for step in pieces:
        kd_copy(*step).wait_send()
    for far in range(planes):
        for sub in range(SUBS):

            @pl.when((tp < planes - 1) & (tp >= far))
            def _():
                z_chunk(tp - far, sub, True).wait_send()

            @pl.when((tp > 0) & (tp + far < planes))
            def _():
                z_chunk(tp + far, sub, False).wait_send()

    @pl.when(grp == 0)
    def _():
        for step in pieces:
            kx_copy(*step).wait_send()


def fused(planes, hidden, w_query, w_key, w_value, prompt_len, page_table):
    rows, model = hidden.shape[1:]
    depth, width = w_query.shape
    half = width // 2
    block = rows // 2
    dma = pltpu.SemaphoreType.DMA
    anywhere = pl.BlockSpec(memory_space=pltpu.HBM)
    result = pl.pallas_call(
        functools.partial(fused_kernel, planes),
        out_shape=jax.ShapeDtypeStruct((rows, width), jnp.bfloat16),
        in_specs=[anywhere] * 6,
        out_specs=anywhere,
        scratch_shapes=[
            pltpu.VMEM((1, prompt_len.shape[0]), jnp.int32),
            pltpu.VMEM(page_table.shape[::-1], jnp.int32),
            pltpu.VMEM((SUBS, rows // planes // SUBS, 2 * depth), jnp.bfloat16),
            pltpu.VMEM((rows, 2 * depth), jnp.bfloat16),
            pltpu.VMEM((rows, 2 * depth), jnp.bfloat16),
            pltpu.VMEM((3, 2 * depth, width), jnp.bfloat16),
            pltpu.VMEM((2, 3, rows, half), jnp.float32),
            pltpu.VMEM((2, 2, rows, half), jnp.float32),
            pltpu.VMEM((2, 2, rows, half), jnp.float32),
            pltpu.VMEM((2, rows, half), jnp.bfloat16),
            pltpu.VMEM((2, rows, half), jnp.bfloat16),
            pltpu.VMEM((2, rows, half), jnp.bfloat16),
            pltpu.VMEM((2, 2, rows, half), jnp.bfloat16),
            pltpu.VMEM((2, 4 * rows, half), jnp.bfloat16),
            pltpu.VMEM((2, rows, 4 * rows), jnp.float32),
            pltpu.VMEM((2, block, half), jnp.bfloat16),
            pltpu.VMEM((2, block, half), jnp.bfloat16),
            dma((6 + SUBS,)), dma((3,)), dma((3,)),
            dma((SUBS,)), dma((SUBS,)), dma((planes * SUBS,)), dma((planes * SUBS,)), dma((planes * SUBS,)),
            dma((18,)), dma((18,)),
            dma((12,)), dma((12,)), dma((12,)), dma((12,)),
            dma((2,)), dma((2,)), dma((2,)),
        ],
        compiler_params=pltpu.CompilerParams(
            collective_id=0, has_side_effects=True, vmem_limit_bytes=67043328
        ),
    )(hidden, w_query, w_key, w_value, prompt_len.reshape(1, -1), page_table.T)
    return result[None]


def solution(mesh):
    planes = mesh.shape["tp"]
    paired = mesh.shape["grp"] == 2 and mesh.shape["seq"] == 4 and planes == 4
    return jax.shard_map(
        functools.partial(fused, planes) if paired else on_device,
        mesh=mesh,
        in_specs=(P("grp", "seq", None), P("seq", "tp"), P("seq", "tp"), P("seq", "tp"), P(), P()),
        out_specs=P("grp", "seq", "tp"),
        check_vma=False,
    )
```

```python
import functools
import math

import jax
import jax.numpy as jnp
from jax import lax
from jax.experimental import pallas as pl
from jax.experimental.pallas import tpu as pltpu
from jax.sharding import PartitionSpec as P

HD = 128
PAGE = 16
STEPS = 4


NEG = -1e30


def from_behind(value, axis, steps):
    count = lax.axis_size(axis)
    first, last = (max(0, -steps), min(count, count - steps))
    return lax.ppermute(value, axis, [(source, source + steps) for source in range(first, last)])


def partial_attention(query, keys, values, allowed):
    rows = query.shape[0]
    heads = query.shape[1] // HD
    query_heads = query.reshape(rows, heads, HD)
    key_heads = keys.reshape(keys.shape[0], heads, HD)
    value_heads = values.reshape(values.shape[0], heads, HD)
    scores = jnp.einsum(
        "rhd,shd->hrs", query_heads, key_heads, preferred_element_type=jnp.float32
    ) * HD ** (-0.5)
    scores = jnp.where(allowed[None], scores, NEG)
    top = jnp.max(scores, axis=2)
    weights = jnp.where(allowed[None], jnp.exp(scores - top[:, :, None]), 0.0)
    total = jnp.sum(weights, axis=2)
    summed = jnp.einsum(
        "hrs,shd->rhd",
        weights.astype(jnp.bfloat16),
        value_heads,
        preferred_element_type=jnp.float32,
    )
    return (top, total, summed.reshape(rows, heads * HD))


def rescale(summed, factor):
    rows = summed.shape[0]
    heads = factor.shape[0]
    return (summed.reshape(rows, heads, HD) * factor.T[:, :, None]).reshape(rows, heads * HD)


def combine(first, second):
    top = jnp.maximum(first[0], second[0])
    early = jnp.exp(first[0] - top)
    later = jnp.exp(second[0] - top)
    return (
        top,
        first[1] * early + second[1] * later,
        rescale(first[2], early) + rescale(second[2], later),
    )


def finish(state):
    return rescale(state[2], 1.0 / state[1]).astype(jnp.bfloat16)


def row_mask(tables, lengths, key_pos):
    pages = key_pos // PAGE
    member = jnp.any(tables[:, :, None] == pages[None, None, :], axis=1)
    allowed = member & (key_pos[None, :] < lengths[:, None])
    return jnp.repeat(allowed, STEPS, axis=0)


def blocked(carry, keys, values, query, mask_of):
    count = keys.shape[0]
    block = math.gcd(count, 512)

    def one_block(state, offset):
        piece_keys = lax.dynamic_slice_in_dim(keys, offset, block, 0)
        piece_values = lax.dynamic_slice_in_dim(values, offset, block, 0)
        key_pos = offset + jnp.arange(block)
        return (
            combine(state, partial_attention(query, piece_keys, piece_values, mask_of(key_pos))),
            None,
        )

    offsets = jnp.arange(count // block) * block
    state, unused = lax.scan(one_block, carry, offsets)
    return state


def on_device(hidden, w_query, w_key, w_value, prompt_len, page_table):
    local = hidden[0]
    rows = local.shape[0]
    width = w_query.shape[1]
    heads = width // HD
    seq_index = lax.axis_index("seq")
    is_prompt = lax.axis_index("grp") == 0
    empty = jnp.zeros((rows, width), jnp.float32)
    piece = (
        lax.all_gather(w_query, "seq", axis=0, tiled=True),
        lax.all_gather(w_key, "seq", axis=0, tiled=True),
        lax.all_gather(w_value, "seq", axis=0, tiled=True),
    )
    projected = tuple(
        (jnp.dot(local, weight, preferred_element_type=jnp.float32) for weight in piece)
    )
    query, keys, values = [item.astype(jnp.bfloat16) for item in projected]
    positions = seq_index * rows + jnp.arange(rows)
    start_state = (
        jnp.full((heads, rows), NEG, jnp.float32),
        jnp.zeros((heads, rows), jnp.float32),
        empty,
    )
    given_keys, given_values = from_behind((keys, values), "grp", 1)
    cache_keys = jnp.where(is_prompt, keys, given_keys)
    cache_values = jnp.where(is_prompt, values, given_values)
    row_count = rows // STEPS
    own_tables = lax.dynamic_slice_in_dim(page_table, seq_index * row_count, row_count, 0)
    own_lengths = lax.dynamic_slice_in_dim(prompt_len, seq_index * row_count, row_count, 0)

    def mask_of(key_pos):
        causal = key_pos[None, :] <= positions[:, None]
        listed = row_mask(own_tables, own_lengths, key_pos)
        return jnp.where(is_prompt, causal, listed)

    piece = (
        lax.all_gather(cache_keys, "seq", axis=0, tiled=True),
        lax.all_gather(cache_values, "seq", axis=0, tiled=True),
    )
    state = blocked(start_state, piece[0], piece[1], query, mask_of)
    frame_row = positions // STEPS
    own_rows = (frame_row[:, None] == frame_row[None, :]) & (
        positions[None, :] <= positions[:, None]
    )
    fresh = partial_attention(query, keys, values, own_rows)
    prefill_out = finish(state)
    decode_out = finish(combine(state, fresh))
    return jnp.where(is_prompt, prefill_out, decode_out)[None]


QUERY, KEY, VALUE = 0, 1, 2
OWN, OTHER = 0, 1
SUBS = 2


def fused_kernel(
    planes, hidden, w_query, w_key, w_value, lengths_in, tables_in, out,
    lengths, tables, stage, own, other, weights, acc, wide_out, wide_in, value_out, value_in, qbuf, fresh, cache, bias, osend, oself,
    local_sem, w_send, w_recv, hy_send, hy_recv, up_send, down_send, hz_recv, p_send, p_recv,
    kx_send, kx_recv, kd_send, kd_recv, o_send, o_recv, o_keep,
):
    inputs = {QUERY: w_query, KEY: w_key, VALUE: w_value}
    rows = hidden.shape[1]
    depth, width = w_query.shape
    span = 2 * depth
    half = width // 2
    heads = half // HD
    block = rows // 2
    chunk = rows // planes // SUBS
    grp = lax.axis_index("grp")
    seq = lax.axis_index("seq")
    tp = lax.axis_index("tp")
    y = seq // 2
    core = seq % 2
    side = tp // (planes // 2)
    partner = {"seq": 2 * y + 1 - core}
    across = {"seq": 2 * (1 - y) + core}
    beside = {"grp": 1 - grp}
    above = {"tp": lax.rem(tp + 1, planes)}
    below = {"tp": lax.rem(tp + planes - 1, planes)}
    kinds = {KEY: 0, VALUE: 1}
    seqs = [2 * y + core, 2 * (1 - y) + core]
    my_heads = pl.ds(pl.multiple_of(y * half, half), half)
    their_heads = pl.ds(pl.multiple_of((1 - y) * half, half), half)
    plane_rows = rows // planes
    starts = (side * block, (planes // 2 - side) * plane_rows, (planes - 1) * (1 - side) * plane_rows)
    sizes = (block, plane_rows, plane_rows)
    parts = [pl.ds(pl.multiple_of(start, plane_rows), size) for start, size in zip(starts, sizes)]

    def remote(src, dst, send, recv, to):
        return pltpu.make_async_remote_copy(
            src_ref=src, dst_ref=dst, send_sem=send, recv_sem=recv,
            device_id=to, device_id_type=pl.DeviceIdType.MESH,
        )

    my_depth = pl.ds(pl.multiple_of(core * depth, depth), depth)
    keeps = {m: pltpu.make_async_copy(inputs[m], weights.at[m, my_depth], local_sem.at[m]) for m in inputs}
    table_keep = pltpu.make_async_copy(tables_in, tables, local_sem.at[3])
    length_keep = pltpu.make_async_copy(lengths_in, lengths, local_sem.at[4])
    own_keep = pltpu.make_async_copy(
        hidden.at[0, :, pl.ds(pl.multiple_of(y * span, span), span)], own, local_sem.at[5]
    )
    def staged(sub):
        take = pl.ds(pl.multiple_of((tp * SUBS + sub) * chunk, chunk), chunk)
        return pltpu.make_async_copy(
            hidden.at[0, take, pl.ds(pl.multiple_of((1 - y) * span, span), span)], stage.at[sub],
            local_sem.at[6 + sub],
        )

    barrier = pltpu.get_barrier_semaphore()
    for peer in (across, partner, beside):
        pl.semaphore_signal(barrier, inc=1, device_id=peer, device_id_type=pl.DeviceIdType.MESH)

    @pl.when(tp < planes - 1)
    def _():
        pl.semaphore_signal(barrier, inc=1, device_id=above, device_id_type=pl.DeviceIdType.MESH)

    @pl.when(tp > 0)
    def _():
        pl.semaphore_signal(barrier, inc=1, device_id=below, device_id_type=pl.DeviceIdType.MESH)

    for sub in range(SUBS):
        staged(sub).start()
    for m in (KEY, VALUE, QUERY):
        keeps[m].start()
    own_keep.start()
    table_keep.start()
    length_keep.start()
    ends = jnp.where(tp == 0, 1, 0) + jnp.where(tp == planes - 1, 1, 0)
    pl.semaphore_wait(barrier, 5 - ends)

    def chunk_rows(plane, sub):
        return pl.ds(pl.multiple_of((plane * SUBS + sub) * chunk, chunk), chunk)

    def y_chunk(sub):
        take = chunk_rows(tp, sub)
        return remote(
            stage.at[sub], other.at[take],
            hy_send.at[sub], hy_recv.at[sub], across,
        )

    def z_chunk(plane, sub, up):
        take = chunk_rows(plane, sub)
        at = plane * SUBS + sub
        return remote(
            other.at[take], other.at[take], (up_send if up else down_send).at[at], hz_recv.at[at],
            above if up else below,
        )

    sent = []

    def launch(copy):
        copy.start()
        sent.append(copy)

    for sub in range(SUBS):
        staged(sub).wait()
        launch(y_chunk(sub))
    swaps = {
        m: remote(weights.at[m, my_depth], weights.at[m, my_depth], w_send.at[m], w_recv.at[m], partner) for m in inputs
    }
    for m in (KEY, VALUE, QUERY):
        keeps[m].wait()
        launch(swaps[m])

    table_keep.wait()
    length_keep.wait()
    total_rows = tables.shape[1]
    keys = cache.shape[1]
    pages = keys // PAGE
    decode_rows = rows // STEPS
    step_bits = STEPS.bit_length() - 1
    page_bits = PAGE.bit_length() - 1
    prompt_one = jnp.where(grp == 0, 1, 0)
    contract_last = (((1,), (1,)), ((), ()))
    table = tables[...]
    page_row = lax.broadcasted_iota(jnp.int32, (pages, total_rows), 0)
    member = table[0:1, :] == page_row
    for listed in range(1, table.shape[0]):
        member = member | (table[listed : listed + 1, :] == page_row)
    member = jnp.where(member, 1.0, 0.0).astype(jnp.bfloat16)
    unfold = lax.broadcasted_iota(jnp.int32, (keys, pages), 1) == lax.shift_right_logical(
        lax.broadcasted_iota(jnp.int32, (keys, pages), 0), page_bits
    )
    unfold = jnp.where(unfold, 1.0, 0.0).astype(jnp.bfloat16)
    seen = jnp.dot(unfold, member, preferred_element_type=jnp.float32)
    key_pos = lax.broadcasted_iota(jnp.int32, (keys, total_rows), 0)
    seen = jnp.where(key_pos < lengths[...], seen, 0.0).astype(jnp.bfloat16)
    for s in (OWN, OTHER):
        spread = (
            lax.shift_right_logical(lax.broadcasted_iota(jnp.int32, (rows, total_rows), 0), step_bits)
            + seqs[s] * decode_rows
            == lax.broadcasted_iota(jnp.int32, (rows, total_rows), 1)
        )
        spread = jnp.where(spread, 1.0, 0.0).astype(jnp.bfloat16)
        listed = lax.dot_general(spread, seen, contract_last, preferred_element_type=jnp.float32)
        causal = (
            lax.broadcasted_iota(jnp.int32, (rows, keys), 1)
            <= lax.broadcasted_iota(jnp.int32, (rows, keys), 0) + seqs[s] * rows
        )
        allowed = jnp.where(prompt_one == 1, jnp.where(causal, 1.0, 0.0), listed)
        bias[s] = jnp.where(allowed > 0.5, 0.0, NEG)

    def project(source, at, m, lanes):
        return jnp.dot(source[at, :], weights[m, :, lanes], preferred_element_type=jnp.float32)

    def part_at(wide, narrow, s, m, at):
        return narrow.at[s, at] if m == VALUE else wide.at[s, m, at]

    def send(source, s, at, m):
        spot = part_at(wide_out, value_out, s, m, at)
        spot[...] = project(source, at, m, their_heads).astype(spot.dtype)

    def keep(source, s, at, m):
        acc[s, m, at] = project(source, at, m, my_heads)

    def both(source, s, at, m):
        send(source, s, at, m)
        keep(source, s, at, m)

    def partial(s, m, piece):
        at = parts[piece]
        number = (s * 3 + m) * 3 + piece
        return remote(
            part_at(wide_out, value_out, s, m, at), part_at(wide_in, value_in, 1 - s, m, at),
            p_send.at[number], p_recv.at[number], across,
        )

    everything = pl.ds(0, rows)

    def pass_on(plane, sub, up, down):
        if up:

            @pl.when(tp < planes - 1)
            def _():
                z_chunk(plane, sub, True).start()

        if down:

            @pl.when(tp > 0)
            def _():
                z_chunk(plane, sub, False).start()

    def take_y(sub):
        y_chunk(sub).wait_recv()
        pass_on(tp, sub, True, True)

    def take_z(far):
        for sub in range(SUBS):

            @pl.when(tp + far < planes)
            def _():
                z_chunk(tp + far, sub, False).wait_recv()
                pass_on(tp + far, sub, False, True)

            @pl.when(tp >= far)
            def _():
                z_chunk(tp - far, sub, True).wait_recv()
                pass_on(tp - far, sub, True, False)

    own_keep.wait()
    for at, m in enumerate((KEY, VALUE, QUERY)):
        swaps[m].wait_recv()
        if at < SUBS:
            take_y(at)
        for piece in range(3):
            send(own, OWN, parts[piece], m)
            if m != QUERY:
                launch(partial(OWN, m, piece))
        keep(own, OWN, everything, m)
    for sub in range(3, SUBS):
        take_y(sub)

    def arrived(s, m, piece):
        at = parts[piece]
        remote(
            part_at(wide_out, value_out, s, m, at), part_at(wide_in, value_in, s, m, at),
            p_send.at[((1 - s) * 3 + m) * 3 + piece], p_recv.at[((1 - s) * 3 + m) * 3 + piece], across,
        ).wait_recv()

    def settled(s, m, piece):
        at = parts[piece]
        far = part_at(wide_in, value_in, s, m, at)[...]
        return (acc[s, m, at] + far.astype(jnp.float32)).astype(jnp.bfloat16)

    def place(s, piece, of_core):
        first = (seqs[s] - core + of_core) * rows + starts[piece]
        return pl.ds(pl.multiple_of(first, plane_rows), sizes[piece])

    pieces = [(s, piece, m) for s in (OTHER, OWN) for piece in range(3) for m in (KEY, VALUE)]

    def number_of(s, piece, m):
        return (s * 3 + piece) * 2 + kinds[m]

    def kx_copy(s, piece, m):
        spot = cache.at[kinds[m], place(s, piece, core)]
        at = number_of(s, piece, m)
        return remote(spot, spot, kx_send.at[at], kx_recv.at[at], beside)

    def kd_copy(s, piece, m):
        spot = cache.at[kinds[m], place(s, piece, core)]
        at = number_of(s, piece, m)
        return remote(spot, spot, kd_send.at[at], kd_recv.at[at], partner)

    def settle(s, piece):
        for m in (KEY, VALUE):
            arrived(s, m, piece)
            fresh[kinds[m], s, parts[piece]] = settled(s, m, piece)

        @pl.when(grp == 0)
        def _():
            for m in (KEY, VALUE):
                cache[kinds[m], place(s, piece, core)] = settled(s, m, piece)
            for m in (KEY, VALUE):
                kx_copy(s, piece, m).start()
                kd_copy(s, piece, m).start()

    def relay(s, piece):
        @pl.when(grp != 0)
        def _():
            for m in (KEY, VALUE):
                kx_copy(s, piece, m).wait_recv()
                kd_copy(s, piece, m).start()

    def others(piece):
        for m in (KEY, VALUE):
            send(other, OTHER, parts[piece], m)
            launch(partial(OTHER, m, piece))
        for m in (KEY, VALUE):
            keep(other, OTHER, parts[piece], m)

    def take_query(s):
        for piece in range(3):
            arrived(s, QUERY, piece)
            qbuf[s, parts[piece]] = settled(s, QUERY, piece)

    take_z(1)
    others(0)
    take_z(2)
    others(1)
    launch(partial(OWN, QUERY, 0))
    launch(partial(OWN, QUERY, 1))
    settle(OTHER, 0)
    settle(OTHER, 1)
    settle(OWN, 0)
    relay(OTHER, 0)
    take_z(3)
    for m in (KEY, VALUE):
        send(other, OTHER, parts[2], m)
        launch(partial(OTHER, m, 2))
    launch(partial(OWN, QUERY, 2))
    for piece in range(3):
        send(other, OTHER, parts[piece], QUERY)
        launch(partial(OTHER, QUERY, piece))
    for m in (KEY, VALUE):
        keep(other, OTHER, parts[2], m)
    settle(OTHER, 2)
    relay(OTHER, 1)
    settle(OWN, 1)
    keep(other, OTHER, everything, QUERY)
    relay(OTHER, 2)
    relay(OWN, 0)
    settle(OWN, 2)
    relay(OWN, 1)
    take_query(OTHER)
    relay(OWN, 2)
    for s, piece, m in pieces:
        spot = cache.at[kinds[m], place(s, piece, 1 - core)]
        at = number_of(s, piece, m)
        remote(spot, spot, kd_send.at[at], kd_recv.at[at], partner).wait_recv()

    fresh_row = lax.broadcasted_iota(jnp.int32, (block, block), 0)
    fresh_col = lax.broadcasted_iota(jnp.int32, (block, block), 1)
    same = (
        lax.shift_right_logical(fresh_row, step_bits) == lax.shift_right_logical(fresh_col, step_bits)
    ) & (fresh_col <= fresh_row)
    fresh_bias = jnp.where(jnp.where(same, 1 - prompt_one, 0) == 1, 0.0, NEG)
    scale = HD ** (-0.5)

    def attend(s, piece, head):
        at = slice(piece * block, (piece + 1) * block)
        lanes = slice(head * HD, (head + 1) * HD)
        query = qbuf[s, at, lanes]

        def scored(key_block, mask):
            return lax.dot_general(
                query, key_block, contract_last, preferred_element_type=jnp.float32
            ) * scale + mask

        scores = [scored(cache[0, :, lanes], bias[s, at]), scored(fresh[0, s, at, lanes], fresh_bias)]
        values = [cache[1, :, lanes], fresh[1, s, at, lanes]]
        top = jnp.maximum(
            jnp.max(scores[0], axis=1, keepdims=True), jnp.max(scores[1], axis=1, keepdims=True)
        )
        total = jnp.zeros((block, 1), jnp.float32)
        summed = jnp.zeros((block, HD), jnp.float32)
        for score, value in zip(scores, values):
            weight = jnp.exp(score - top)
            total += jnp.sum(weight, axis=1, keepdims=True)
            summed += jnp.dot(weight.astype(jnp.bfloat16), value, preferred_element_type=jnp.float32)
        return (summed / total).astype(jnp.bfloat16)

    def out_copy(piece):
        span = pl.ds(piece * block, block)
        return remote(osend.at[piece], out.at[span, my_heads], o_send.at[piece], o_recv.at[piece], across)

    def out_keep(piece):
        span = pl.ds(piece * block, block)
        return pltpu.make_async_copy(oself.at[piece], out.at[span, my_heads], o_keep.at[piece])

    for piece in range(2):
        for head in range(heads):
            osend[piece, :, head * HD : (head + 1) * HD] = attend(OTHER, piece, head)
        launch(out_copy(piece))
    take_query(OWN)
    for piece in range(2):
        for head in range(heads):
            oself[piece, :, head * HD : (head + 1) * HD] = attend(OWN, piece, head)
        out_keep(piece).start()
    for piece in range(2):
        span = pl.ds(piece * block, block)
        remote(osend.at[piece], out.at[span, their_heads], o_send.at[piece], o_recv.at[piece], across).wait_recv()
        out_keep(piece).wait()

    for copy in sent:
        copy.wait_send()
    for step in pieces:
        kd_copy(*step).wait_send()
    for far in range(planes):
        for sub in range(SUBS):

            @pl.when((tp < planes - 1) & (tp >= far))
            def _():
                z_chunk(tp - far, sub, True).wait_send()

            @pl.when((tp > 0) & (tp + far < planes))
            def _():
                z_chunk(tp + far, sub, False).wait_send()

    @pl.when(grp == 0)
    def _():
        for step in pieces:
            kx_copy(*step).wait_send()


def fused(planes, hidden, w_query, w_key, w_value, prompt_len, page_table):
    rows, model = hidden.shape[1:]
    depth, width = w_query.shape
    half = width // 2
    block = rows // 2
    dma = pltpu.SemaphoreType.DMA
    anywhere = pl.BlockSpec(memory_space=pltpu.HBM)
    result = pl.pallas_call(
        functools.partial(fused_kernel, planes),
        out_shape=jax.ShapeDtypeStruct((rows, width), jnp.bfloat16),
        in_specs=[anywhere] * 6,
        out_specs=anywhere,
        scratch_shapes=[
            pltpu.VMEM((1, prompt_len.shape[0]), jnp.int32),
            pltpu.VMEM(page_table.shape[::-1], jnp.int32),
            pltpu.VMEM((SUBS, rows // planes // SUBS, 2 * depth), jnp.bfloat16),
            pltpu.VMEM((rows, 2 * depth), jnp.bfloat16),
            pltpu.VMEM((rows, 2 * depth), jnp.bfloat16),
            pltpu.VMEM((3, 2 * depth, width), jnp.bfloat16),
            pltpu.VMEM((2, 3, rows, half), jnp.float32),
            pltpu.VMEM((2, 2, rows, half), jnp.float32),
            pltpu.VMEM((2, 2, rows, half), jnp.float32),
            pltpu.VMEM((2, rows, half), jnp.bfloat16),
            pltpu.VMEM((2, rows, half), jnp.bfloat16),
            pltpu.VMEM((2, rows, half), jnp.bfloat16),
            pltpu.VMEM((2, 2, rows, half), jnp.bfloat16),
            pltpu.VMEM((2, 4 * rows, half), jnp.bfloat16),
            pltpu.VMEM((2, rows, 4 * rows), jnp.float32),
            pltpu.VMEM((2, block, half), jnp.bfloat16),
            pltpu.VMEM((2, block, half), jnp.bfloat16),
            dma((6 + SUBS,)), dma((3,)), dma((3,)),
            dma((SUBS,)), dma((SUBS,)), dma((planes * SUBS,)), dma((planes * SUBS,)), dma((planes * SUBS,)),
            dma((18,)), dma((18,)),
            dma((12,)), dma((12,)), dma((12,)), dma((12,)),
            dma((2,)), dma((2,)), dma((2,)),
        ],
        compiler_params=pltpu.CompilerParams(
            collective_id=0, has_side_effects=True, vmem_limit_bytes=67043328
        ),
    )(hidden, w_query, w_key, w_value, prompt_len.reshape(1, -1), page_table.T)
    return result[None]


def solution(mesh):
    planes = mesh.shape["tp"]
    paired = mesh.shape["grp"] == 2 and mesh.shape["seq"] == 4 and planes == 4
    return jax.shard_map(
        functools.partial(fused, planes) if paired else on_device,
        mesh=mesh,
        in_specs=(P("grp", "seq", None), P("seq", "tp"), P("seq", "tp"), P("seq", "tp"), P(), P()),
        out_specs=P("grp", "seq", "tp"),
        check_vma=False,
    )
```
